32 devices in a mesh: seq: 8 (over z, y), fsdp: 4 (over x, core).
Axes of the slice: x: 2, y: 2, z: 4, core: 2. Of those that a mesh axis runs over, the one named last changes fastest.
Arguments:
- inputs: bfloat16 [4, 1024, 2560], P('fsdp', 'seq'), may hold values from -6 to 6
- gain_first: float32 [2560], replicated, may hold values from 0.5 to 1.5
- branch_weight: bfloat16 [5120, 2560], P(('seq', 'fsdp')), may hold values from -0.125 to 0.125
- branch_bias: float32 [5120], replicated, may hold values from -3 to 3
- conv_weight: float32 [4, 2560], replicated, may hold values from -3 to 3
- conv_bias: float32 [2560], replicated, may hold values from -2 to 2
- gate_weight: bfloat16 [2, 10, 256, 256], replicated, may hold values from -0.375 to 0.375
- gate_bias: float32 [2, 2560], replicated, may hold values from -4 to 4
- decay: float32 [2560], replicated, may hold values from -12 to -3.8
- out_weight: bfloat16 [2560, 2560], P(('seq', 'fsdp')), may hold values from -0.25 to 0.25
- out_bias: float32 [2560], replicated, may hold values from -2 to 2
- gain_second: float32 [2560], replicated, may hold values from 0.5 to 1.5
- mlp_weight: bfloat16 [15360, 2560], P(('seq', 'fsdp')), may hold values from -0.125 to 0.125
- down_weight: bfloat16 [2560, 7680], P(('seq', 'fsdp')), may hold values from -0.125 to 0.125
- cotangent: bfloat16 [4, 1024, 2560], P('fsdp', 'seq'), may hold values from -6 to 6
Outputs:
- output: bfloat16 [4, 1024, 2560], P('fsdp', 'seq')
- input_grad: float32 [4, 1024, 2560], P('fsdp', 'seq')
- gain_first_grad: float32 [2560], replicated
- branch_weight_grad: float32 [5120, 2560], P(('seq', 'fsdp'))
- branch_bias_grad: float32 [5120], replicated
- conv_weight_grad: float32 [4, 2560], replicated
- conv_bias_grad: float32 [2560], replicated
- gate_weight_grad: float32 [2, 10, 256, 256], replicated
- gate_bias_grad: float32 [2, 2560], replicated
- decay_grad: float32 [2560], replicated
- out_weight_grad: float32 [2560, 2560], P(('seq', 'fsdp'))
- out_bias_grad: float32 [2560], replicated
- gain_second_grad: float32 [2560], replicated
- mlp_weight_grad: float32 [15360, 2560], P(('seq', 'fsdp'))
- down_weight_grad: float32 [2560, 7680], P(('seq', 'fsdp'))
The draws below stay inside these ranges and needn't reach their ends.
All inputs are finite; a program needn't handle non-finite values.
Results may differ from the reference program's by a relative error of at most 0.014.
Values may be sent and summed in bfloat16 or wider, within the bound.
A program may use at most 384 MiB of HBM per device.

```python
import jax
import jax.numpy as jnp
from jax import lax

D = 2560
FF = 7680
HEADS = 10
TAPS = 4
BLOCK = 256
SEQS = 4
LENGTH = 1024


def draw_decay(key, part):
    key_slow, key_rate = jax.random.split(key, 2)
    slow_share = 0.5
    slow = jax.random.uniform(key_slow, (D,), jnp.float32) < slow_share
    spread = jax.random.uniform(key_rate, (D,), jnp.float32)
    low_slow = jnp.log(0.1 / LENGTH)
    high_slow = jnp.log(0.5 / LENGTH)
    high_fast = jnp.log(0.02)
    slow_rate = jnp.exp(low_slow + spread * (high_slow - low_slow))
    fast_rate = jnp.exp(high_slow + spread * (high_fast - high_slow))
    rate = jnp.where(slow, slow_rate, fast_rate)
    return jnp.log(jnp.expm1(rate)).astype(jnp.float32)


def steps_of(own_key, dims, pieces, least, top_value):
    level, own = 1.0, jax.random.fold_in(own_key, 6)
    for axis_at, shards_of in pieces:
        steps = jnp.exp(jax.random.uniform(jax.random.fold_in(own, axis_at), (shards_of,), jnp.float32, least / len(pieces), top_value / len(pieces)))
        level = level * jnp.repeat(steps, dims[axis_at] // shards_of).reshape([-1 if axis == axis_at else 1 for axis in range(len(dims))])
    return level


def bell_draw(own_key, shape, scale, bound, pieces=(), kind=jnp.bfloat16):
    array = jax.random.normal(own_key, shape, jnp.float32) * scale
    if len(pieces) > 0:
        array = steps_of(own_key, shape, pieces, -0.22, 0.18) * array
    return jnp.clip(array, min=-bound, max=bound).astype(kind)


def setup_inputs(seed: int = 0) -> dict:
    splits = jax.random.split(jax.random.key(seed), 16)
    return {
        "inputs": bell_draw(splits[0], (SEQS, LENGTH, D), 1.0, 6.0, ((0, 4), (1, 8))),
        "gain_first": jnp.clip(1.0 + 0.1 * jax.random.normal(splits[1], (D,), jnp.float32), 0.5, 1.5),
        "branch_weight": bell_draw(splits[2], (2 * D, D), D ** -0.5, 0.125, ((0, 32),)),
        "branch_bias": bell_draw(splits[3], (2 * D,), 0.5, 3.0, (), jnp.float32),
        "conv_weight": bell_draw(splits[4], (TAPS, D), 0.5, 3.0, (), jnp.float32),
        "conv_bias": bell_draw(splits[5], (D,), 0.3, 2.0, (), jnp.float32),
        "gate_weight": bell_draw(splits[6], (2, HEADS, BLOCK, BLOCK), BLOCK ** -0.5, 0.375),
        "gate_bias": bell_draw(splits[7], (2, D), 1.0, 4.0, (), jnp.float32),
        "decay": draw_decay(jax.random.fold_in(splits[15], 71), 0),
        "out_weight": bell_draw(splits[9], (D, D), (D // 4) ** -0.5, 0.25, ((0, 32),)),
        "out_bias": bell_draw(splits[10], (D,), 0.3, 2.0, (), jnp.float32),
        "gain_second": jnp.clip(1.0 + 0.1 * jax.random.normal(splits[11], (D,), jnp.float32), 0.5, 1.5),
        "mlp_weight": bell_draw(splits[12], (2 * FF, D), D ** -0.5, 0.125, ((0, 32),)),
        "down_weight": bell_draw(splits[13], (D, FF), (FF // 4) ** -0.5, 0.125, ((0, 32),)),
        "cotangent": bell_draw(splits[14], (SEQS, LENGTH, D), 1.0, 6.0, ((0, 4), (1, 8))),
    }


@jax.custom_vjp
def low(v):
    return lax.optimization_barrier(v.astype(jnp.bfloat16)).astype(jnp.float32)

@jax.custom_vjp
def low_back(v):
    return v

def low_keep(v):
    return (low(v), None)

def low_pass(kept, grad):
    return (grad,)

def back_keep(v):
    return (v, None)

def back_low(kept, grad):
    return (low(grad),)
low.defvjp(low_keep, low_pass)
low_back.defvjp(back_keep, back_low)
epsilon = 1e-06
highest = lax.Precision.HIGHEST

def normed(values, scales):
    return values * lax.rsqrt(lax.optimization_barrier(jnp.mean(values * values, -1, keepdims=True)) + epsilon) * scales

def product(operand, weight):
    return jnp.dot(operand, weight.T, precision=highest)

def affine(earlier, latter):
    return (latter[0] * earlier[0], latter[0] * earlier[1] + latter[1])

def lru_inputs(gates, decay, conv_out, opening):
    rgate = jax.nn.sigmoid(gates[0])
    igate = jax.nn.sigmoid(gates[1])
    log_rate = -8.0 * jax.nn.softplus(decay) * rgate
    decays = jnp.exp(log_rate)
    scaling = jnp.where(opening, 1.0, jnp.sqrt(-jnp.expm1(2.0 * log_rate)))
    return (decays, scaling * igate * conv_out)

def one_sequence(source, params):
    gain_first, branch_weight, branch_bias, conv_weight, conv_bias, gate_weight, gate_bias, decay, out_weight, out_bias, gain_second, mlp_weight, down_weight = params
    tap_count = conv_weight.shape[0]
    opening = (jnp.arange(LENGTH) == 0)[:, None]
    first_in = low(normed(source, gain_first))
    branch_pre = low_back(product(first_in, branch_weight) + branch_bias)
    gate_pre = branch_pre[:, :D]
    conv_in = branch_pre[:, D:]
    gelu_gate = jax.nn.gelu(gate_pre, approximate=True)
    padded = jnp.pad(conv_in, ((tap_count - 1, 0), (0, 0)))
    conv_out = conv_bias + jnp.zeros_like(conv_in)
    for lagged in range(tap_count):
        conv_out = conv_out + conv_weight[lagged] * padded[tap_count - 1 - lagged:tap_count - 1 - lagged + LENGTH]
    conv_low = low(conv_out).reshape(LENGTH, HEADS, BLOCK)
    gates = jnp.einsum('lhb,ghbc->glhc', conv_low, gate_weight, precision=highest).reshape(2, LENGTH, D)
    gates = low_back(gates + gate_bias[:, None, :])
    decays, drive = lru_inputs(gates, decay, conv_out, opening)
    states = lax.associative_scan(affine, (decays, drive), axis=0)[1]
    mixed = low(states * gelu_gate)
    middle = source + low_back(product(mixed, out_weight) + out_bias)
    second_in = low(normed(middle, gain_second))
    mlp_pre = low_back(product(second_in, mlp_weight))
    mlp_hidden = low(jax.nn.gelu(mlp_pre[:, :FF], approximate=True) * mlp_pre[:, FF:])
    return middle + low_back(product(mlp_hidden, down_weight))

def reference(inputs, gain_first, branch_weight, branch_bias, conv_weight, conv_bias, gate_weight, gate_bias, decay, out_weight, out_bias, gain_second, mlp_weight, down_weight, cotangent):
    params = tuple((value.astype(jnp.float32) for value in (gain_first, branch_weight, branch_bias, conv_weight, conv_bias, gate_weight, gate_bias, decay, out_weight, out_bias, gain_second, mlp_weight, down_weight)))

    def forward(source, *weights):
        return lax.map(lambda single: one_sequence(single, weights), source)
    result, backward = jax.vjp(forward, inputs.astype(jnp.float32), *params)
    gradient = backward(cotangent.astype(jnp.float32))
    return (result.astype(jnp.bfloat16), gradient[0], gradient[1], gradient[2], gradient[3], gradient[4], gradient[5], gradient[6], gradient[7], gradient[8], gradient[9], gradient[10], gradient[11], gradient[12], gradient[13])
```

```python
import functools

import jax
import jax.numpy as jnp
from jax import lax
from jax.experimental import pallas as pl
from jax.experimental.pallas import tpu as pltpu
from jax.sharding import Mesh
from jax.sharding import PartitionSpec as P

epsilon = 1e-06
low = jnp.bfloat16
wide = jnp.float32

cube = ("b3", "b2", "b1", "b0")
block_size = 16
places = ("g",) + cube
seq_axes = ("g", "b3", "b2")
fsdp_axes = ("b1", "b0")
orders = (("b3", "b1", "b2"), ("b3", "b2", "b1"))
back_orders = (("b1", "b2", "b3"), ("b2", "b1", "b3"))

anywhere = pl.BlockSpec(memory_space=pl.ANY)
in_vmem = pl.BlockSpec(memory_space=pltpu.VMEM)
in_smem = pl.BlockSpec(memory_space=pltpu.SMEM)
whole_vmem = 67000000


def bit_of(axis):
    return 1 << (len(cube) - 1 - cube.index(axis))


def slot_at(mask):
    slot = 0
    for axis in cube:
        here = lax.axis_index(axis)
        slot = slot * 2 + (1 - here if mask & bit_of(axis) else here)
    return slot


def device_at(mask):
    return {axis: 1 - lax.axis_index(axis) for axis in cube if mask & bit_of(axis)}


def greet(masks):
    barrier = pltpu.get_barrier_semaphore()
    for mask in masks:
        pl.semaphore_signal(
            barrier, inc=1, device_id=device_at(mask), device_id_type=pl.DeviceIdType.MESH
        )
    pl.semaphore_wait(barrier, len(masks))


def split_rows(rows, unit):
    tiles = rows // unit
    sizes = [(tiles + 1 - part) // 2 * unit for part in range(2)]
    return [(part, part * sizes[0], size) for part, size in enumerate(sizes) if size > 0]


def remote_params(collective):
    return pltpu.CompilerParams(
        collective_id=collective, has_side_effects=True, vmem_limit_bytes=whole_vmem
    )


def gather_kernel(pieces, x_ref, out_ref, send_sem, recv_sem, local_sem):
    greet([bit_of(axis) for axis in cube])
    sent = []

    def push(part, start, size, mask, axis):
        slot = slot_at(mask)
        source = (x_ref if mask == 0 else out_ref.at[slot]).at[pl.ds(start, size)]
        copy = pltpu.make_async_remote_copy(
            src_ref=source,
            dst_ref=out_ref.at[slot].at[pl.ds(start, size)],
            send_sem=send_sem.at[len(sent)],
            recv_sem=recv_sem.at[part, mask ^ bit_of(axis)],
            device_id=device_at(bit_of(axis)),
            device_id_type=pl.DeviceIdType.MESH,
        )
        copy.start()
        sent.append(copy)

    def arrive(part, start, size, mask):
        target = out_ref.at[slot_at(mask)].at[pl.ds(start, size)]
        pltpu.make_async_copy(target, target, recv_sem.at[part, mask]).wait()

    own = pltpu.make_async_copy(x_ref, out_ref.at[slot_at(0)], local_sem)
    own.start()
    for stage in range(4):
        for part, start, size in pieces:
            order = orders[part] + ("b0",)
            masks = [0]
            if stage > 0:
                for axis in order[: stage - 1]:
                    masks = masks + [mask | bit_of(axis) for mask in masks]
                masks = [mask | bit_of(order[stage - 1]) for mask in masks]
            for mask in masks:
                if mask:
                    arrive(part, start, size, mask)
                for axis in order[stage:]:
                    push(part, start, size, mask, axis)
    for part, start, size in pieces:
        for mask in range(block_size):
            if mask & bit_of("b0"):
                arrive(part, start, size, mask)
    for copy in sent:
        copy.wait_send()
    own.wait()


def block_gather(values, collective):
    rows, width = values.shape
    pieces = split_rows(rows, 16)
    return pl.pallas_call(
        functools.partial(gather_kernel, pieces),
        out_shape=jax.ShapeDtypeStruct((block_size, rows, width), values.dtype),
        in_specs=[in_vmem],
        out_specs=anywhere,
        scratch_shapes=[
            pltpu.SemaphoreType.DMA((15 * len(pieces),)),
            pltpu.SemaphoreType.DMA((2, block_size)),
            pltpu.SemaphoreType.DMA,
        ],
        compiler_params=remote_params(collective),
        name="block_gather",
    )(values)


def scatter_kernel(pieces, source_count, *refs):
    sources = refs[:source_count]
    out_ref, own, away, send_sem, recv_sem, load_sem = refs[source_count:]
    core = bit_of("b0")
    greet([bit_of(axis) for axis in cube])
    sent = []

    def push(source, number, hop, index, axis):
        _, _, _, start, size = pieces[number]
        copy = pltpu.make_async_remote_copy(
            src_ref=source,
            dst_ref=away.at[hop, index].at[pl.ds(start, size)],
            send_sem=send_sem.at[len(sent)],
            recv_sem=recv_sem.at[number, hop, index],
            device_id=device_at(bit_of(axis)),
            device_id_type=pl.DeviceIdType.MESH,
        )
        copy.start()
        sent.append(copy)

    def sequence(order):
        first, second, third = (bit_of(axis) for axis in back_orders[order])
        return [
            first | second | third,
            first | second,
            first | third,
            first,
            second | third,
            second,
            third,
            0,
        ]

    def arrive(number, hop, index):
        _, _, _, start, size = pieces[number]
        target = away.at[hop, index].at[pl.ds(start, size)]
        pltpu.make_async_copy(target, target, recv_sem.at[number, hop, index]).wait()

    loads = {}
    for turn in range(8):
        for number, (order, source, begin, start, size) in enumerate(pieces):
            mask = sequence(order)[turn]
            rows = pl.ds(begin, size)
            push(
                sources[source].at[slot_at(mask | core)].at[rows], number, 0, mask >> 1, "b0"
            )
    for turn in range(8):
        for number, (order, source, begin, start, size) in enumerate(pieces):
            mask = sequence(order)[turn]
            load = pltpu.make_async_copy(
                sources[source].at[slot_at(mask)].at[pl.ds(begin, size)],
                own.at[mask >> 1].at[pl.ds(start, size)],
                load_sem.at[number, mask >> 1],
            )
            load.start()
            loads[number, mask] = load
    for turn in range(8):
        for number, (order, source, begin, start, size) in enumerate(pieces):
            mask = sequence(order)[turn]
            index = mask >> 1
            bits = [bit_of(axis) for axis in back_orders[order]]
            loads[number, mask].wait()
            hops = [0]
            arrive(number, 0, index)
            target = None
            for hop, bit in enumerate(bits):
                if mask & bit:
                    target = hop
                    break
                arrive(number, hop + 1, index)
                hops.append(hop + 1)

            def add_tile(i, carry, index=index, start=start, hops=hops, target=target):
                at = pl.ds(pl.multiple_of(start + i * 16, 16), 16)
                total = own[index, at, :].astype(wide)
                for hop in hops:
                    total = total + away[hop, index, at, :].astype(wide)
                if target is None:
                    out_ref[at, :] = total.astype(out_ref.dtype)
                else:
                    own[index, at, :] = total.astype(own.dtype)
                return carry

            lax.fori_loop(0, size // 16, add_tile, 0)
            if target is not None:
                push(
                    own.at[index].at[pl.ds(start, size)],
                    number,
                    target + 1,
                    (mask ^ bits[target]) >> 1,
                    back_orders[order][target],
                )
    for copy in sent:
        copy.wait_send()


def block_scatter(collective, *partials):
    width = partials[0].shape[2]
    pieces = []
    rows = 0
    for source, partial in enumerate(partials):
        for order, begin, size in split_rows(partial.shape[1], 16):
            pieces.append((order, source, begin, rows + begin, size))
        rows += partial.shape[1]
    return pl.pallas_call(
        functools.partial(scatter_kernel, pieces, len(partials)),
        out_shape=jax.ShapeDtypeStruct((rows, width), wide),
        in_specs=[anywhere] * len(partials),
        out_specs=in_vmem,
        scratch_shapes=[
            pltpu.VMEM((8, rows, width), low),
            pltpu.VMEM((4, 8, rows, width), low),
            pltpu.SemaphoreType.DMA((15 * len(pieces),)),
            pltpu.SemaphoreType.DMA((len(pieces), 4, 8)),
            pltpu.SemaphoreType.DMA((len(pieces), 8)),
        ],
        compiler_params=remote_params(collective),
        name="block_scatter",
    )(*partials)


def swap_kernel(x_ref, out_ref, send_sem, recv_sem, local_sem):
    greet(list(range(1, block_size)))
    sent = []
    here = slot_at(0)
    for mask in (15, 14, 13, 11, 7, 12, 10, 6, 9, 5, 3, 8, 4, 2, 1):
        copy = pltpu.make_async_remote_copy(
            src_ref=x_ref.at[slot_at(mask)],
            dst_ref=out_ref.at[here],
            send_sem=send_sem.at[mask],
            recv_sem=recv_sem.at[mask],
            device_id=device_at(mask),
            device_id_type=pl.DeviceIdType.MESH,
        )
        copy.start()
        sent.append(copy)
    own = pltpu.make_async_copy(x_ref.at[here], out_ref.at[here], local_sem)
    own.start()
    for mask in range(1, block_size):
        target = out_ref.at[slot_at(mask)]
        pltpu.make_async_copy(target, target, recv_sem.at[mask]).wait()
    for copy in sent:
        copy.wait_send()
    own.wait()


def block_swap(values, collective):
    return pl.pallas_call(
        swap_kernel,
        out_shape=jax.ShapeDtypeStruct(values.shape, values.dtype),
        in_specs=[in_vmem],
        out_specs=in_vmem,
        scratch_shapes=[
            pltpu.SemaphoreType.DMA((block_size,)),
            pltpu.SemaphoreType.DMA((block_size,)),
            pltpu.SemaphoreType.DMA,
        ],
        compiler_params=remote_params(collective),
        name="block_swap",
    )(values)


def group_gather(values):
    return lax.all_gather(values, "g", axis=0)


def group_sum(partials):
    return lax.psum_scatter(partials.astype(low), "g", scatter_dimension=0).astype(wide)


def group_total(values):
    count = lax.axis_size("g")
    total = values
    for distance in range(1, count):
        route = [(i, (i + distance) % count) for i in range(count)]
        total = total + lax.ppermute(values.astype(low), "g", route).astype(wide)
    return total


def spread_kernel(group_count, x_ref, out_ref, send_sem, recv_sem, local_sem):
    here_g, here_3, here_2 = (lax.axis_index(axis) for axis in seq_axes)
    peers = []
    for step in range(group_count):
        for mask in range(4):
            if step or mask:
                peers.append((step, mask))

    def place(step, mask):
        return (
            lax.rem(here_g + step, group_count),
            1 - here_3 if mask & 2 else here_3,
            1 - here_2 if mask & 1 else here_2,
        )

    barrier = pltpu.get_barrier_semaphore()
    for step, mask in peers:
        pl.semaphore_signal(
            barrier,
            inc=1,
            device_id=dict(zip(seq_axes, place(step, mask))),
            device_id_type=pl.DeviceIdType.MESH,
        )
    pl.semaphore_wait(barrier, len(peers))
    mine = here_g * 4 + here_3 * 2 + here_2
    sent = []
    for number, (step, mask) in enumerate(peers):
        copy = pltpu.make_async_remote_copy(
            src_ref=x_ref,
            dst_ref=out_ref.at[mine],
            send_sem=send_sem.at[number],
            recv_sem=recv_sem.at[number],
            device_id=dict(zip(seq_axes, place(step, mask))),
            device_id_type=pl.DeviceIdType.MESH,
        )
        copy.start()
        sent.append(copy)
    own = pltpu.make_async_copy(x_ref, out_ref.at[mine], local_sem)
    own.start()
    for number, (step, mask) in enumerate(peers):
        from_g, from_3, from_2 = place(group_count - step, mask)
        target = out_ref.at[from_g * 4 + from_3 * 2 + from_2]
        pltpu.make_async_copy(target, target, recv_sem.at[number]).wait()
    for copy in sent:
        copy.wait_send()
    own.wait()


def seq_spread(values, collective):
    group_count = lax.axis_size("g")
    count = 4 * group_count
    return pl.pallas_call(
        functools.partial(spread_kernel, group_count),
        out_shape=jax.ShapeDtypeStruct((count,) + values.shape, values.dtype),
        in_specs=[in_vmem],
        out_specs=in_vmem,
        scratch_shapes=[
            pltpu.SemaphoreType.DMA((count,)),
            pltpu.SemaphoreType.DMA((count,)),
            pltpu.SemaphoreType.DMA,
        ],
        compiler_params=remote_params(collective),
        name="seq_spread",
    )(values)


def rim_rows(values, offset):
    count = 4 * lax.axis_size("g")
    route = [(i - offset, i) for i in range(count) if 0 <= i - offset < count]
    return lax.ppermute(values, seq_axes, route)


def gelu_parts(v):
    inner = 0.7978845608028654 * (v + 0.044715 * v * v * v)
    t = jnp.tanh(inner)
    value = 0.5 * v * (1.0 + t)
    slope = 0.5 * (1.0 + t) + 0.5 * v * (1.0 - t * t) * 0.7978845608028654 * (
        1.0 + 0.134145 * v * v
    )
    return value, slope


def shifted(values, distance, fill):
    rows = values.shape[0]
    if distance % 8 == 0:
        head = jnp.full((distance,) + values.shape[1:], fill, values.dtype)
        return jnp.concatenate([head, values[: rows - distance]], 0)
    row = lax.broadcasted_iota(jnp.int32, values.shape, 0)
    return jnp.where(row >= distance, pltpu.roll(values, distance, 0), fill)


def shifted_back(values, distance, fill):
    rows = values.shape[0]
    if distance % 8 == 0:
        tail = jnp.full((distance,) + values.shape[1:], fill, values.dtype)
        return jnp.concatenate([values[distance:], tail], 0)
    row = lax.broadcasted_iota(jnp.int32, values.shape, 0)
    return jnp.where(row < rows - distance, pltpu.roll(values, rows - distance, 0), fill)


def scan_rows(rates, terms, shift):
    distance = 1
    while distance < rates.shape[0]:
        terms = terms + rates * shift(terms, distance, 0.0)
        rates = rates * shift(rates, distance, 1.0)
        distance *= 2
    return rates, terms


def one_minus_square(log_rate):
    x = 2.0 * log_rate
    series = 1.0
    for n in (9, 8, 7, 6, 5, 4, 3, 2):
        series = 1.0 + x * (1.0 / n) * series
    return jnp.where(x > -0.5, -x * series, 1.0 - jnp.exp(x))


def lagged_sum(ext, weights, start):
    total = start
    for lag in range(weights.shape[0]):
        moved = pltpu.roll(ext, lag, 0) if lag else ext
        total = total + weights[lag : lag + 1, :] * moved[8:, :]
    return total


def opening_rows(shape, position):
    return (lax.broadcasted_iota(jnp.int32, shape, 0) == 0) & (position == 0)


def local_states_kernel(
    position_ref,
    conv_in_ref,
    before_ref,
    taps_ref,
    bias_ref,
    weight_ref,
    gate_bias_ref,
    rate_ref,
    conv_out_ref,
    rgate_ref,
    igate_ref,
    decay_ref,
    local_ref,
    product_ref,
    ends_ref,
):
    ext = jnp.concatenate([before_ref[...], conv_in_ref[...]], 0)
    conv_out = lagged_sum(ext, taps_ref[...], bias_ref[...])
    conv_low = conv_out.astype(low)
    gates = [
        jax.nn.sigmoid(
            jnp.dot(conv_low, weight_ref[j, 0], preferred_element_type=wide)
            + gate_bias_ref[j : j + 1, :]
        )
        for j in range(2)
    ]
    log_rate = rate_ref[...] * gates[0]
    rates = jnp.exp(log_rate)
    scaling = jnp.where(
        opening_rows(rates.shape, position_ref[0]), 1.0, jnp.sqrt(one_minus_square(log_rate))
    )
    product, states = scan_rows(rates, scaling * gates[1] * conv_out, shifted)
    conv_out_ref[...] = conv_out
    rgate_ref[...] = gates[0]
    igate_ref[...] = gates[1]
    decay_ref[...] = rates
    local_ref[...] = states
    product_ref[...] = product
    rows = rates.shape[0]
    ends_ref[...] = jnp.concatenate(
        [
            product[rows - 1 :],
            states[rows - 1 :],
        ],
        0,
    )


def full_states_kernel(
    position_ref, local_ref, product_ref, ends_ref, gate_pre_ref, states_ref, mixed_ref, entry_ref
):
    entry = jnp.zeros((1, local_ref.shape[1]), wide)
    for s in range(ends_ref.shape[0]):
        later = ends_ref[s, 0:1, :] * entry + ends_ref[s, 1:2, :]
        entry = jnp.where(s < position_ref[0], later, entry)
    states = local_ref[...] + product_ref[...] * entry
    states_ref[...] = states
    mixed_ref[...] = (states * gelu_parts(gate_pre_ref[...])[0]).astype(low)
    entry_ref[...] = jnp.broadcast_to(entry, entry_ref.shape)


def local_adjoint_kernel(
    grad_mixed_ref, gate_pre_ref, decay_ref, local_ref, product_ref, ends_ref
):
    grad_states = grad_mixed_ref[...] * gelu_parts(gate_pre_ref[...])[0]
    rates = decay_ref[...]
    product, adjoint = scan_rows(shifted_back(rates, 1, 1.0), grad_states, shifted_back)
    local_ref[...] = adjoint
    product_ref[...] = product
    ends_ref[...] = jnp.concatenate(
        [
            rates[0:1] * product[0:1],
            rates[0:1] * adjoint[0:1],
        ],
        0,
    )


def gate_grads_kernel(
    position_ref,
    local_ref,
    product_ref,
    ends_ref,
    decay_ref,
    rgate_ref,
    igate_ref,
    conv_out_ref,
    states_ref,
    entry_ref,
    conv_in_ref,
    before_ref,
    weight_ref,
    rate_ref,
    grad_conv_ref,
    weight_grad_ref,
    sums_ref,
):
    position = position_ref[0]
    entry = jnp.zeros((1, local_ref.shape[1]), wide)
    for s in range(ends_ref.shape[0] - 1, 0, -1):
        earlier = ends_ref[s, 0:1, :] * entry + ends_ref[s, 1:2, :]
        entry = jnp.where(s > position, earlier, entry)
    adjoint = local_ref[...] + product_ref[...] * entry
    rates = decay_ref[...]
    rgate = rgate_ref[...]
    igate = igate_ref[...]
    conv_out = conv_out_ref[...]
    row = lax.broadcasted_iota(jnp.int32, rates.shape, 0)
    before = jnp.where(row == 0, entry_ref[0:1, :], pltpu.roll(states_ref[...], 1, 0))
    opening = opening_rows(rates.shape, position)
    log_rate = rate_ref[...] * rgate
    root = jnp.sqrt(one_minus_square(log_rate))
    scaling = jnp.where(opening, 1.0, root)
    grad_scaling = adjoint * igate * conv_out
    grad_log = adjoint * before * rates - jnp.where(
        opening, 0.0, grad_scaling * rates * rates / root
    )
    grad_rgate = grad_log * rate_ref[...] * rgate * (1.0 - rgate)
    grad_igate = adjoint * scaling * conv_out * igate * (1.0 - igate)
    grad_conv = adjoint * scaling * igate
    conv_low = conv_out.astype(low)
    sums = []
    for j, grad in enumerate((grad_rgate, grad_igate)):
        grad_low = grad.astype(low)
        sums.append(jnp.sum(grad_low.astype(wide), 0, keepdims=True))
        weight_grad_ref[j, 0] = lax.dot_general(
            conv_low, grad_low, (((0,), (0,)), ((), ())), preferred_element_type=wide
        )
        grad_conv = grad_conv + lax.dot_general(
            grad_low, weight_ref[j, 0], (((1,), (1,)), ((), ())), preferred_element_type=wide
        )
    grad_conv_ref[...] = grad_conv
    sums.append(jnp.sum(grad_log * rgate, 0, keepdims=True))
    sums.append(jnp.sum(grad_conv, 0, keepdims=True))
    ext = jnp.concatenate([before_ref[...], conv_in_ref[...]], 0)
    for lag in range(4):
        moved = pltpu.roll(ext, lag, 0) if lag else ext
        sums.append(jnp.sum(grad_conv * moved[8:, :], 0, keepdims=True))
    sums_ref[...] = jnp.concatenate(sums, 0)


def branch_grads_kernel(
    grad_conv_ref, after_ref, taps_ref, gate_pre_ref, grad_mixed_ref, states_ref, out_ref, sums_ref
):
    grad_conv = grad_conv_ref[...]
    rows = grad_conv.shape[0]
    ext = jnp.concatenate([grad_conv, after_ref[...]], 0)
    total = taps_ref[0:1, :] * grad_conv
    for lag in range(1, taps_ref.shape[0]):
        moved = pltpu.roll(ext, rows + 8 - lag, 0)
        total = total + taps_ref[lag : lag + 1, :] * moved[:rows, :]
    slope = gelu_parts(gate_pre_ref[...])[1]
    grad_gate = slope * grad_mixed_ref[...] * states_ref[...]
    sums = []
    for j, grad in enumerate((grad_gate, total)):
        grad_low = grad.astype(low)
        out_ref[j] = grad_low
        sums.append(jnp.sum(grad_low.astype(wide), 0, keepdims=True))
    sums_ref[...] = jnp.concatenate(sums + [jnp.zeros((6, grad_conv.shape[1]), wide)], 0)


def by_heads(kernel, heads, width, operands, outs, name):
    def spec(shape):
        if len(shape) == 1:
            return in_smem
        if len(shape) == 4:
            return pl.BlockSpec((shape[0], 1, width, width), lambda h: (0, h, 0, 0))
        lead = shape[:-1]
        return pl.BlockSpec(lead + (width,), lambda h, rank=len(lead): (0,) * rank + (h,))

    return pl.pallas_call(
        kernel,
        grid=(heads,),
        out_shape=[jax.ShapeDtypeStruct(shape, dtype) for shape, dtype in outs],
        in_specs=[spec(value.shape) for value in operands],
        out_specs=[spec(shape) for shape, _ in outs],
        compiler_params=pltpu.CompilerParams(vmem_limit_bytes=48000000),
        name=name,
    )(*operands)


def normed(values, scales):
    return values * lax.rsqrt(jnp.mean(values * values, -1, keepdims=True) + epsilon) * scales


def gated_unit(gate, up):
    return jax.nn.gelu(gate, approximate=True) * up


def times_rows(operand, weight):
    return lax.dot_general(
        operand, weight, (((1,), (1,)), ((), ())), preferred_element_type=wide
    )


def times(operand, weight):
    return jnp.dot(operand, weight, preferred_element_type=wide)


def row_sums(gradient, operand):
    return lax.dot_general(
        gradient, operand, (((0,), (0,)), ((), ())), preferred_element_type=wide
    )


def gain_sums(gradient, weight):
    return jnp.sum(gradient * weight.astype(wide), 0)


def member_columns(values):
    rows, width = values.shape
    count = lax.axis_size("g")
    split = values.reshape(rows, count, block_size, width // (count * block_size))
    return split.transpose(2, 0, 1, 3).reshape(block_size, rows, width // block_size)


def body(
    inputs,
    gain_first,
    branch_weight,
    branch_bias,
    conv_weight,
    conv_bias,
    gate_weight,
    gate_bias,
    decay,
    out_weight,
    out_bias,
    gain_second,
    mlp_weight,
    down_weight,
    cotangent,
):
    source = inputs[0].astype(wide)
    rows, width = source.shape
    heads, head_width = gate_weight.shape[1:3]
    count = lax.axis_size("g")
    half = count // 2
    all_rows = block_size * rows
    position = (
        lax.axis_index("g") * 4 + lax.axis_index("b3") * 2 + lax.axis_index("b2")
    ).reshape(1)
    flat = (rows, width)
    small = (8, width)

    branch_rows = group_gather(branch_weight).reshape(-1, width)
    mlp_rows = group_gather(mlp_weight)
    gate_rows = mlp_rows[:half].reshape(-1, width)
    up_rows = mlp_rows[half:].reshape(-1, width)
    down_rows, hidden_width = down_weight.shape
    unit = hidden_width // (half * block_size)
    down_split = (
        down_weight.reshape(down_rows, half, block_size, unit)
        .transpose(2, 0, 1, 3)
        .reshape(block_size, down_rows, half * unit)
    )
    down_columns = group_gather(block_swap(down_split, 0)).reshape(width, half * unit)
    out_rows = lax.all_gather(out_weight, places, axis=0, tiled=True)

    first_in = normed(source, gain_first).astype(low)
    first_all = block_gather(first_in, 1).reshape(all_rows, width)
    grad_out = cotangent[0]
    cot_all = block_gather(grad_out, 12).reshape(all_rows, width)
    pre_part = times_rows(first_all, branch_rows).astype(low)
    pre_part = pre_part.reshape(block_size, rows, 2 * width // block_size)
    pre = block_swap(pre_part, 2).reshape(block_size, rows, count, -1)
    pre = pre.transpose(1, 2, 0, 3).reshape(rows, 2 * width).astype(wide) + branch_bias
    gate_pre = pre[:, :width]
    conv_in = pre[:, width:]
    conv_before = rim_rows(conv_in[rows - 8 :], 1)

    rate = (-8.0 * jax.nn.softplus(decay))[None]
    conv_out, rgate, igate, decays, local, product, ends = by_heads(
        local_states_kernel,
        heads,
        head_width,
        (
            position,
            conv_in,
            conv_before,
            conv_weight,
            conv_bias[None],
            gate_weight,
            gate_bias,
            rate,
        ),
        [(flat, wide)] * 6 + [((2, width), wide)],
        "local_states",
    )
    states, mixed, entry = by_heads(
        full_states_kernel,
        heads,
        head_width,
        (position, local, product, seq_spread(ends, 3), gate_pre),
        [(flat, wide), (flat, low), (small, wide)],
        "full_states",
    )
    mixed_all = lax.all_gather(mixed, cube, axis=0, tiled=True)
    middle = source + times_rows(mixed, out_rows) + out_bias

    grad_hidden = times(cot_all, down_columns)
    second_in = normed(middle, gain_second).astype(low)
    second_all = block_gather(second_in, 4).reshape(all_rows, width)
    mlp_gate = times_rows(second_all, gate_rows)
    mlp_up = times_rows(second_all, up_rows)
    mlp_hidden, gated_back = jax.vjp(gated_unit, mlp_gate, mlp_up)
    mlp_hidden = mlp_hidden.astype(low)
    grad_gate, grad_up = (grad.astype(low) for grad in gated_back(grad_hidden))
    second_part = times(grad_gate, gate_rows) + times(grad_up, up_rows)
    grad_second = block_scatter(5, second_part.astype(low).reshape(block_size, rows, width))
    down_part = times_rows(mlp_hidden, down_columns).astype(low)
    down_part = down_part.reshape(block_size, rows, width)

    gate_sum = row_sums(grad_gate, second_all)
    up_sum = row_sums(grad_up, second_all)
    mlp_sum = jnp.concatenate([gate_sum.astype(low), up_sum.astype(low)], 0)
    mlp_grad = group_sum(mlp_sum.reshape(count, -1, width))
    gain_second_term = gain_sums(gate_sum, gate_rows) + gain_sums(up_sum, up_rows)
    gain_second_term = gain_second_term / gain_second
    down_sum = row_sums(cot_all, mlp_hidden)
    down_sum = group_sum(down_sum.reshape(count, block_size, down_rows, half * unit))
    down_grad = (
        block_swap(down_sum.astype(low), 7)
        .reshape(block_size, down_rows, half, unit)
        .transpose(1, 2, 0, 3)
        .reshape(down_rows, hidden_width)
        .astype(wide)
    )

    norm_second, second_back = jax.vjp(lambda values: normed(values, gain_second), middle)
    grad_middle = grad_out.astype(wide) + second_back(grad_second)[0]
    grad_branch = grad_middle.astype(low)
    out_bias_term = jnp.sum(grad_branch.astype(wide), 0)
    grad_mixed = times(grad_branch, out_rows)
    branch_all = block_swap(member_columns(grad_branch), 8).reshape(all_rows, -1)
    out_grad = group_sum(row_sums(branch_all, mixed_all).reshape(count, -1, width))

    adjoint, tail, adjoint_ends = by_heads(
        local_adjoint_kernel,
        heads,
        head_width,
        (grad_mixed, gate_pre, decays),
        [(flat, wide), (flat, wide), ((2, width), wide)],
        "local_adjoint",
    )
    grad_conv, gate_weight_term, gate_sums = by_heads(
        gate_grads_kernel,
        heads,
        head_width,
        (
            position,
            adjoint,
            tail,
            seq_spread(adjoint_ends, 9),
            decays,
            rgate,
            igate,
            conv_out,
            states,
            entry,
            conv_in,
            conv_before,
            gate_weight,
            rate,
        ),
        [(flat, wide), (gate_weight.shape, wide), (small, wide)],
        "gate_grads",
    )
    conv_after = rim_rows(grad_conv[:8], -1)
    pre_grads, pre_sums = by_heads(
        branch_grads_kernel,
        heads,
        head_width,
        (grad_conv, conv_after, conv_weight, gate_pre, grad_mixed, states),
        [((2, rows, width), low), (small, wide)],
        "branch_grads",
    )

    columns = pre_grads.reshape(2, rows, half, block_size, -1).transpose(3, 1, 0, 2, 4)
    pre_all = block_swap(columns.reshape(block_size, rows, -1), 10).reshape(all_rows, -1)
    branch_sum = row_sums(pre_all, first_all)
    branch_grad = group_sum(branch_sum.reshape(count, -1, width))
    gain_first_term = gain_sums(branch_sum, branch_rows) / gain_first
    first_part = times(pre_all, branch_rows).astype(low)

    vectors = jnp.concatenate(
        [
            gain_first_term[None],
            pre_sums[:2],
            gate_sums[4:8],
            gate_sums[3:4],
            gate_sums[:2],
            gate_sums[2:3] * (-8.0 * jax.nn.sigmoid(decay)),
            out_bias_term[None],
            gain_second_term[None],
            jnp.zeros((block_size - 13, width), wide),
        ],
        0,
    ).astype(low)
    gate_terms = gate_weight_term.reshape(block_size, -1, width).astype(low)
    gate_unit = gate_terms.shape[1]
    shared_part = jnp.concatenate(
        [
            gate_terms,
            vectors[:, None, :],
            jnp.zeros((block_size, 15, width), low),
        ],
        1,
    )
    scattered = block_scatter(11, first_part.reshape(block_size, rows, width), shared_part)
    grad_first = scattered[:rows]
    shared = group_total(scattered[rows:]).astype(low)
    norm_first, first_back = jax.vjp(lambda values: normed(values, gain_first), source)
    input_grad = (grad_middle + first_back(grad_first)[0])[None]

    down_part, shared = lax.optimization_barrier((down_part, shared))
    down_full = block_scatter(6, down_part)
    output = (middle + down_full).astype(low)[None]
    shared_all = block_gather(shared, 13).astype(wide)
    gate_weight_grad = shared_all[:, :gate_unit].reshape(gate_weight.shape)
    sums = shared_all[:, gate_unit]
    return (
        output,
        input_grad,
        sums[0],
        branch_grad,
        sums[1:3].reshape(-1),
        sums[3:7],
        sums[7],
        gate_weight_grad,
        sums[8:10],
        sums[10],
        out_grad,
        sums[11],
        sums[12],
        mlp_grad,
        down_grad,
    )


def solution(mesh):
    count = mesh.devices.size // block_size
    blocks = Mesh(mesh.devices.reshape((count,) + (2,) * len(cube)), places)
    tokens = P(fsdp_axes, seq_axes, None)
    owned = P(places, None)
    return jax.shard_map(
        body,
        mesh=blocks,
        in_specs=(
            tokens,
            P(),
            owned,
            P(),
            P(),
            P(),
            P(),
            P(),
            P(),
            owned,
            P(),
            P(),
            owned,
            owned,
            tokens,
        ),
        out_specs=(
            tokens,
            tokens,
            P(),
            owned,
            P(),
            P(),
            P(),
            P(),
            P(),
            P(),
            owned,
            P(),
            P(),
            owned,
            owned,
        ),
        check_vma=False,
    )
```

```python
import functools

import jax
import jax.numpy as jnp
from jax import lax
from jax.experimental import pallas as pl
from jax.experimental.pallas import tpu as pltpu
from jax.sharding import Mesh
from jax.sharding import PartitionSpec as P

epsilon = 1e-06
low = jnp.bfloat16
wide = jnp.float32

cube = ("b3", "b2", "b1", "b0")
block_size = 16
places = ("g",) + cube
seq_axes = ("g", "b3", "b2")
fsdp_axes = ("b1", "b0")
first_orders = (("b3", "b1", "b2"), ("b3", "b2", "b1"))
even_orders = (("b1", "b3", "b2"), ("b2", "b3", "b1"))

anywhere = pl.BlockSpec(memory_space=pl.ANY)
in_vmem = pl.BlockSpec(memory_space=pltpu.VMEM)
in_smem = pl.BlockSpec(memory_space=pltpu.SMEM)
whole_vmem = 67000000


def bit_of(axis):
    return 1 << (len(cube) - 1 - cube.index(axis))


def slot_at(mask):
    slot = 0
    for axis in cube:
        here = lax.axis_index(axis)
        slot = slot * 2 + (1 - here if mask & bit_of(axis) else here)
    return slot


def device_at(mask):
    return {axis: 1 - lax.axis_index(axis) for axis in cube if mask & bit_of(axis)}


def greet(masks, paired):
    barrier = pltpu.get_barrier_semaphore()
    targets = [device_at(mask) for mask in masks] + [other_block()] * paired
    for target in targets:
        pl.semaphore_signal(
            barrier, inc=1, device_id=target, device_id_type=pl.DeviceIdType.MESH
        )
    pl.semaphore_wait(barrier, len(targets))


def other_block():
    return {"g": 1 - lax.axis_index("g")}


class Ride:
    def __init__(self, riders):
        self.arrays = [array for array, _, _ in riders]
        self.ranges = [(start, size) for _, start, size in riders]
        self.chunks = []
        for number, (array, start, size) in enumerate(riders):
            step = 16 if array.shape[1] > 4096 else (48 if array.shape[1] > 1024 else 160)
            for begin in range(0, size, step):
                self.chunks.append((number, start + begin, begin, min(step, size - begin)))

    def shapes(self):
        return [
            jax.ShapeDtypeStruct((size,) + array.shape[1:], array.dtype)
            for array, (_, size) in zip(self.arrays, self.ranges)
        ]

    def semaphores(self):
        count = max(1, len(self.chunks))
        return [pltpu.SemaphoreType.DMA((count,)), pltpu.SemaphoreType.DMA((count,))]

    def enter(self, inputs, outputs, send_sem, recv_sem):
        self.copies = [
            pltpu.make_async_remote_copy(
                src_ref=inputs[number].at[pl.ds(begin, size)],
                dst_ref=outputs[number].at[pl.ds(start, size)],
                send_sem=send_sem.at[chunk],
                recv_sem=recv_sem.at[chunk],
                device_id=other_block(),
                device_id_type=pl.DeviceIdType.MESH,
            )
            for chunk, (number, begin, start, size) in enumerate(self.chunks)
        ]
        self.started = 0

    def start(self, share):
        until = -(-len(self.copies) * share[0] // share[1])
        for copy in self.copies[self.started : until]:
            copy.start()
        self.started = max(self.started, until)

    def finish(self):
        self.start((1, 1))
        for copy in self.copies:
            copy.wait()


def split_rows(rows, orders):
    tiles = rows // 16
    pieces = []
    start = 0
    for number, order in enumerate(orders):
        size = (tiles + len(orders) - 1 - number) // len(orders) * 16
        if size:
            pieces.append((order, start, size))
        start += size
    return pieces


def hop_orders(riders):
    return first_orders + even_orders if riders else even_orders


def remote_params(collective, held):
    return pltpu.CompilerParams(
        collective_id=collective,
        has_side_effects=True,
        vmem_limit_bytes=min(whole_vmem, held + (2 << 20)),
    )


def bytes_of(*values):
    return sum(value.size * value.dtype.itemsize for value in values)


def move_kernel(pieces, swap_count, ride, *refs):
    refs = list(refs)

    def take(count):
        taken = refs[:count]
        del refs[:count]
        return taken

    gathers = 1 if pieces else 0
    count = len(ride.arrays)
    sources, swaps, riders = take(gathers), take(swap_count), take(count)
    targets, swapped, arrivals = take(gathers), take(swap_count), take(count)
    send_sem, recv_sem, local_sem, swap_send, swap_recv, ride_send, ride_recv = refs
    neighbours = [bit_of(axis) for axis in cube]
    greet(list(range(1, block_size)) if swap_count else neighbours, count > 0)
    ride.enter(riders, arrivals, ride_send, ride_recv)
    sent = []
    here = slot_at(0)
    locals_ = []

    def push(part, start, size, mask, axis):
        slot = slot_at(mask)
        source = (sources[0] if mask == 0 else targets[0].at[slot]).at[pl.ds(start, size)]
        copy = pltpu.make_async_remote_copy(
            src_ref=source,
            dst_ref=targets[0].at[slot].at[pl.ds(start, size)],
            send_sem=send_sem.at[len(sent)],
            recv_sem=recv_sem.at[part, mask ^ bit_of(axis)],
            device_id=device_at(bit_of(axis)),
            device_id_type=pl.DeviceIdType.MESH,
        )
        copy.start()
        sent.append(copy)

    def arrive(part, start, size, mask):
        target = targets[0].at[slot_at(mask)].at[pl.ds(start, size)]
        pltpu.make_async_copy(target, target, recv_sem.at[part, mask]).wait()

    def forward(stage):
        for part, (order, start, size) in enumerate(pieces):
            order = order + ("b0",)
            masks = [0]
            if stage > 0:
                for axis in order[: stage - 1]:
                    masks = masks + [mask | bit_of(axis) for mask in masks]
                masks = [mask | bit_of(order[stage - 1]) for mask in masks]
            for mask in masks:
                if mask:
                    arrive(part, start, size, mask)
                for axis in order[stage:]:
                    push(part, start, size, mask, axis)

    forward(0)
    swap_copies = []
    for mask in (15, 14, 13, 11, 7, 12, 10, 6, 9, 5, 3, 8, 4, 2, 1):
        for number in range(swap_count):
            copy = pltpu.make_async_remote_copy(
                src_ref=swaps[number].at[slot_at(mask)],
                dst_ref=swapped[number].at[here],
                send_sem=swap_send.at[number, mask],
                recv_sem=swap_recv.at[number, mask],
                device_id=device_at(mask),
                device_id_type=pl.DeviceIdType.MESH,
            )
            copy.start()
            swap_copies.append(copy)
    ride.start((1, 1))
    for number in range(gathers):
        locals_.append((sources[number], targets[number].at[here]))
    for number in range(swap_count):
        locals_.append((swaps[number].at[here], swapped[number].at[here]))
    locals_ = [
        pltpu.make_async_copy(source, target, local_sem.at[number])
        for number, (source, target) in enumerate(locals_)
    ]
    for copy in locals_:
        copy.start()
    for stage in (1, 2, 3):
        forward(stage)
    for part, (_, start, size) in enumerate(pieces):
        for mask in range(block_size):
            if mask & bit_of("b0"):
                arrive(part, start, size, mask)
    for number in range(swap_count):
        for mask in range(1, block_size):
            target = swapped[number].at[slot_at(mask)]
            pltpu.make_async_copy(target, target, swap_recv.at[number, mask]).wait()
    for copy in sent + swap_copies:
        copy.wait_send()
    for copy in locals_:
        copy.wait()
    ride.finish()


def block_move(gathered, swapped, collective, riders=()):
    pieces = []
    shapes = []
    gathers = [] if gathered is None else [gathered]
    for values in gathers:
        pieces = split_rows(values.shape[0], hop_orders(riders))
        shapes.append(jax.ShapeDtypeStruct((block_size,) + values.shape, values.dtype))
    for values in swapped:
        shapes.append(jax.ShapeDtypeStruct(values.shape, values.dtype))
    ride = Ride(riders)
    swaps = max(1, len(swapped))
    moved = len(gathers) * [anywhere] + len(swapped) * [in_vmem] + len(riders) * [anywhere]
    return pl.pallas_call(
        functools.partial(move_kernel, pieces, len(swapped), ride),
        out_shape=shapes + ride.shapes(),
        in_specs=len(gathers) * [in_vmem] + moved[len(gathers) :],
        out_specs=moved,
        scratch_shapes=[
            pltpu.SemaphoreType.DMA((max(1, 15 * len(pieces)),)),
            pltpu.SemaphoreType.DMA((max(1, len(pieces)), block_size)),
            pltpu.SemaphoreType.DMA((1 + swaps,)),
            pltpu.SemaphoreType.DMA((swaps, block_size)),
            pltpu.SemaphoreType.DMA((swaps, block_size)),
        ]
        + ride.semaphores(),
        compiler_params=remote_params(
            collective, 2 * bytes_of(*gathers) + 4 * bytes_of(*swapped)
        ),
        name="block_move",
    )(*gathers, *swapped, *ride.arrays)


def scatter_kernel(pieces, product_rows, transposed, extra_count, ride, *refs):
    refs = list(refs)

    def take(count):
        taken = refs[:count]
        del refs[:count]
        return taken

    products = len(transposed)
    count = len(ride.arrays)
    left_refs, right_refs, extras, riders = (
        take(products),
        take(products),
        take(extra_count),
        take(count),
    )
    (out_ref,), arrivals = take(1), take(count)
    left_rows = take(products)
    held, away, send_sem, recv_sem, left_sem, load_sem, ride_send, ride_recv = refs
    core = bit_of("b0")
    members = 2 * product_rows
    order_count = [sum(mask >> bit & 1 for bit in range(len(cube))) for mask in range(block_size)]
    steps = sorted(
        (mask for mask in range(block_size) if not mask & core),
        key=lambda mask: (-order_count[mask], -mask),
    )
    here = lax.axis_index("b0")

    def left_copy(number, step):
        pair = slot_at(steps[step]) // 2
        rows = pl.ds(pl.multiple_of(pair * members, members), members)
        return pltpu.make_async_copy(
            left_refs[number].at[rows], left_rows[number].at[step], left_sem.at[number, step]
        )

    for step in range(8):
        for number in range(products):
            left_copy(number, step).start()
    greet([bit_of(axis) for axis in cube], count > 0)
    ride.enter(riders, arrivals, ride_send, ride_recv)
    sent = []

    def slot_of(order, hop, mask):
        clear = [bit_of(axis) for axis in order[:hop]] + [core]
        masks = [m for m in range(block_size) if not any(m & bit for bit in clear)]
        return (0, 8, 12, 14)[hop] + masks.index(mask)

    def push(source, number, slot, axis):
        _, _, _, start, size = pieces[number]
        copy = pltpu.make_async_remote_copy(
            src_ref=source,
            dst_ref=away.at[slot].at[pl.ds(start, size)],
            send_sem=send_sem.at[len(sent)],
            recv_sem=recv_sem.at[number, slot],
            device_id=device_at(bit_of(axis)),
            device_id_type=pl.DeviceIdType.MESH,
        )
        copy.start()
        sent.append(copy)

    def arrive(number, slot):
        _, _, _, start, size = pieces[number]
        target = away.at[slot].at[pl.ds(start, size)]
        pltpu.make_async_copy(target, target, recv_sem.at[number, slot]).wait()

    tile = 512

    def work_out(step):
        for number in range(products):
            left_copy(number, step).wait()

        def columns(i, carry):
            at = pl.ds(pl.multiple_of(i * tile, tile), tile)
            total = None
            for number in range(products):
                left = left_rows[number][step]
                if transposed[number]:
                    term = lax.dot_general(
                        left,
                        right_refs[number][at, :],
                        (((1,), (1,)), ((), ())),
                        preferred_element_type=wide,
                    )
                else:
                    term = jnp.dot(left, right_refs[number][:, at], preferred_element_type=wide)
                total = term if total is None else total + term
            total = total.astype(low)
            held[step, 0, pl.ds(0, product_rows), at] = total[:product_rows]
            held[step, 1, pl.ds(0, product_rows), at] = total[product_rows:]
            return carry

        lax.fori_loop(0, out_ref.shape[1] // tile, columns, 0)
        for number, (order, extra, begin, start, size) in enumerate(pieces):
            rows = pl.ds(begin, size)
            if extra:
                source = extras[0].at[slot_at(steps[step] | core)].at[rows]
            else:
                source = held.at[step, 1 - here].at[rows]
            push(source, number, slot_of(order, 0, steps[step]), "b0")

    loads = {}
    for step in range(8):
        for number, (order, extra, begin, start, size) in enumerate(pieces):
            if extra:
                loads[number, step] = pltpu.make_async_copy(
                    extras[0].at[slot_at(steps[step])].at[pl.ds(begin, size)],
                    held.at[step, here].at[pl.ds(start, size)],
                    load_sem.at[number, step],
                )
                loads[number, step].start()

    def pass_on(step):
        mask = steps[step]
        for number, (order, extra, begin, start, size) in enumerate(pieces):
            bits = [bit_of(axis) for axis in order]
            if extra:
                loads[number, step].wait()
            slots = [slot_of(order, 0, mask)]
            target = None
            for hop, bit in enumerate(bits):
                if mask & bit:
                    target = hop
                    break
                slots.append(slot_of(order, hop + 1, mask))
            for slot in slots:
                arrive(number, slot)

            def add_tile(i, carry, start=start, slots=slots, target=target):
                at = pl.ds(pl.multiple_of(start + i * 16, 16), 16)
                total = held[step, here, at, :].astype(wide)
                for slot in slots:
                    total = total + away[slot, at, :].astype(wide)
                if target is None:
                    out_ref[at, :] = total.astype(out_ref.dtype)
                else:
                    held[step, here, at, :] = total.astype(low)
                return carry

            lax.fori_loop(0, size // 16, add_tile, 0)
            if target is not None:
                push(
                    held.at[step, here].at[pl.ds(start, size)],
                    number,
                    slot_of(order, target + 1, mask ^ bits[target]),
                    order[target],
                )

    for step in range(9):
        if step < 8:
            work_out(step)
        if step == 0:
            ride.start((1, 1))
        if step > 0:
            pass_on(step - 1)
    for copy in sent:
        copy.wait_send()
    ride.finish()


def block_scatter(products, collective, riders=(), extra=None):
    ride = Ride(riders)
    lefts = [left for left, _, _ in products]
    rights = [right for _, right, _ in products]
    transposed = [flag for _, _, flag in products]
    product_rows = lefts[0].shape[0] // block_size
    width = rights[0].shape[0] if transposed[0] else rights[0].shape[1]
    extras = [] if extra is None else [extra]
    orders = [order[::-1] for order in hop_orders(riders)]
    pieces = [
        (order, 0, start, start, size) for order, start, size in split_rows(product_rows, orders)
    ]
    rows = product_rows
    for values in extras:
        for order, start, size in split_rows(values.shape[1], orders):
            pieces.append((order, 1, start, rows + start, size))
        rows += values.shape[1]
    padded = [-(-left.shape[1] // 128) * 128 for left in lefts]
    held_bytes = (
        (16 + 15) * rows * width * 2
        + 2 * rows * width * 4
        + sum(2 * left.shape[0] * size for left, size in zip(lefts, padded))
        + 2 * sum(2 * size * width for size in padded)
        + (8 << 20)
    )
    return pl.pallas_call(
        functools.partial(
            scatter_kernel, pieces, product_rows, transposed, len(extras), ride
        ),
        out_shape=[jax.ShapeDtypeStruct((rows, width), wide)] + ride.shapes(),
        in_specs=[anywhere] * len(lefts)
        + [in_vmem] * len(rights)
        + [anywhere] * (len(extras) + len(riders)),
        out_specs=[in_vmem] + [anywhere] * len(riders),
        scratch_shapes=[pltpu.VMEM((8, 2 * product_rows, left.shape[1]), low) for left in lefts]
        + [
            pltpu.VMEM((8, 2, rows, width), low),
            pltpu.VMEM((15, rows, width), low),
            pltpu.SemaphoreType.DMA((15 * len(pieces),)),
            pltpu.SemaphoreType.DMA((len(pieces), 15)),
            pltpu.SemaphoreType.DMA((len(lefts), 8)),
            pltpu.SemaphoreType.DMA((len(pieces), 8)),
        ]
        + ride.semaphores(),
        compiler_params=remote_params(collective, held_bytes),
        name="block_scatter",
    )(*lefts, *rights, *extras, *ride.arrays)


def group_shift(values, distance):
    count = lax.axis_size("g")
    return lax.ppermute(values, "g", [(i, (i + distance) % count) for i in range(count)])


def group_gather(values):
    return lax.all_gather(values, "g", axis=0)


def group_sum(partials):
    return lax.psum_scatter(partials.astype(low), "g", scatter_dimension=0).astype(wide)


def group_total(values):
    count = lax.axis_size("g")
    total = values
    for distance in range(1, count):
        total = total + group_shift(values.astype(low), distance).astype(wide)
    return total


def spread_kernel(group_count, x_ref, out_ref, send_sem, recv_sem, local_sem):
    here_g, here_3, here_2 = (lax.axis_index(axis) for axis in seq_axes)
    peers = []
    for step in range(group_count):
        for mask in range(4):
            if step or mask:
                peers.append((step, mask))

    def place(step, mask):
        return (
            lax.rem(here_g + step, group_count),
            1 - here_3 if mask & 2 else here_3,
            1 - here_2 if mask & 1 else here_2,
        )

    barrier = pltpu.get_barrier_semaphore()
    for step, mask in peers:
        pl.semaphore_signal(
            barrier,
            inc=1,
            device_id=dict(zip(seq_axes, place(step, mask))),
            device_id_type=pl.DeviceIdType.MESH,
        )
    pl.semaphore_wait(barrier, len(peers))
    mine = here_g * 4 + here_3 * 2 + here_2
    sent = []
    for number, (step, mask) in enumerate(peers):
        copy = pltpu.make_async_remote_copy(
            src_ref=x_ref,
            dst_ref=out_ref.at[mine],
            send_sem=send_sem.at[number],
            recv_sem=recv_sem.at[number],
            device_id=dict(zip(seq_axes, place(step, mask))),
            device_id_type=pl.DeviceIdType.MESH,
        )
        copy.start()
        sent.append(copy)
    own = pltpu.make_async_copy(x_ref, out_ref.at[mine], local_sem)
    own.start()
    for number, (step, mask) in enumerate(peers):
        from_g, from_3, from_2 = place(group_count - step, mask)
        target = out_ref.at[from_g * 4 + from_3 * 2 + from_2]
        pltpu.make_async_copy(target, target, recv_sem.at[number]).wait()
    for copy in sent:
        copy.wait_send()
    own.wait()


def seq_spread(values, collective):
    group_count = lax.axis_size("g")
    count = 4 * group_count
    return pl.pallas_call(
        functools.partial(spread_kernel, group_count),
        out_shape=jax.ShapeDtypeStruct((count,) + values.shape, values.dtype),
        in_specs=[in_vmem],
        out_specs=in_vmem,
        scratch_shapes=[
            pltpu.SemaphoreType.DMA((count,)),
            pltpu.SemaphoreType.DMA((count,)),
            pltpu.SemaphoreType.DMA,
        ],
        compiler_params=remote_params(collective, 2 * (count + 1) * 8 * bytes_of(values)),
        name="seq_spread",
    )(values)


def rim_rows(values, offset):
    count = 4 * lax.axis_size("g")
    route = [(i - offset, i) for i in range(count) if 0 <= i - offset < count]
    return lax.ppermute(values, seq_axes, route)


def gelu_parts(v):
    inner = 0.7978845608028654 * (v + 0.044715 * v * v * v)
    t = jnp.tanh(inner)
    value = 0.5 * v * (1.0 + t)
    slope = 0.5 * (1.0 + t) + 0.5 * v * (1.0 - t * t) * 0.7978845608028654 * (
        1.0 + 0.134145 * v * v
    )
    return value, slope


def shifted(values, distance, fill):
    rows = values.shape[0]
    if distance % 8 == 0:
        head = jnp.full((distance,) + values.shape[1:], fill, values.dtype)
        return jnp.concatenate([head, values[: rows - distance]], 0)
    row = lax.broadcasted_iota(jnp.int32, values.shape, 0)
    return jnp.where(row >= distance, pltpu.roll(values, distance, 0), fill)


def shifted_back(values, distance, fill):
    rows = values.shape[0]
    if distance % 8 == 0:
        tail = jnp.full((distance,) + values.shape[1:], fill, values.dtype)
        return jnp.concatenate([values[distance:], tail], 0)
    row = lax.broadcasted_iota(jnp.int32, values.shape, 0)
    return jnp.where(row < rows - distance, pltpu.roll(values, rows - distance, 0), fill)


def scan_rows(rates, terms, shift):
    distance = 1
    while distance < rates.shape[0]:
        terms = terms + rates * shift(terms, distance, 0.0)
        rates = rates * shift(rates, distance, 1.0)
        distance *= 2
    return rates, terms


def one_minus_square(log_rate):
    x = 2.0 * log_rate
    series = 1.0
    for n in (9, 8, 7, 6, 5, 4, 3, 2):
        series = 1.0 + x * (1.0 / n) * series
    return jnp.where(x > -0.5, -x * series, 1.0 - jnp.exp(x))


def lagged_sum(ext, weights, start):
    total = start
    for lag in range(weights.shape[0]):
        moved = pltpu.roll(ext, lag, 0) if lag else ext
        total = total + weights[lag : lag + 1, :] * moved[8:, :]
    return total


def opening_rows(shape, position):
    return (lax.broadcasted_iota(jnp.int32, shape, 0) == 0) & (position == 0)


def local_states_kernel(
    position_ref,
    conv_in_ref,
    before_ref,
    taps_ref,
    bias_ref,
    weight_ref,
    gate_bias_ref,
    rate_ref,
    conv_out_ref,
    rgate_ref,
    igate_ref,
    decay_ref,
    local_ref,
    product_ref,
    ends_ref,
):
    ext = jnp.concatenate([before_ref[...], conv_in_ref[...]], 0)
    conv_out = lagged_sum(ext, taps_ref[...], bias_ref[...])
    conv_low = conv_out.astype(low)
    gates = [
        jax.nn.sigmoid(
            jnp.dot(conv_low, weight_ref[j, 0], preferred_element_type=wide)
            + gate_bias_ref[j : j + 1, :]
        )
        for j in range(2)
    ]
    log_rate = rate_ref[...] * gates[0]
    rates = jnp.exp(log_rate)
    scaling = jnp.where(
        opening_rows(rates.shape, position_ref[0]), 1.0, jnp.sqrt(one_minus_square(log_rate))
    )
    product, states = scan_rows(rates, scaling * gates[1] * conv_out, shifted)
    conv_out_ref[...] = conv_out
    rgate_ref[...] = gates[0]
    igate_ref[...] = gates[1]
    decay_ref[...] = rates
    local_ref[...] = states
    product_ref[...] = product
    rows = rates.shape[0]
    ends_ref[...] = jnp.concatenate(
        [
            product[rows - 1 :],
            states[rows - 1 :],
        ],
        0,
    )


def full_states_kernel(
    position_ref, local_ref, product_ref, ends_ref, gate_pre_ref, states_ref, mixed_ref, entry_ref
):
    entry = jnp.zeros((1, local_ref.shape[1]), wide)
    for s in range(ends_ref.shape[0]):
        later = ends_ref[s, 0:1, :] * entry + ends_ref[s, 1:2, :]
        entry = jnp.where(s < position_ref[0], later, entry)
    states = local_ref[...] + product_ref[...] * entry
    states_ref[...] = states
    mixed_ref[...] = (states * gelu_parts(gate_pre_ref[...])[0]).astype(low)
    entry_ref[...] = jnp.broadcast_to(entry, entry_ref.shape)


def local_adjoint_kernel(
    grad_mixed_ref, gate_pre_ref, decay_ref, local_ref, product_ref, ends_ref
):
    grad_states = grad_mixed_ref[...] * gelu_parts(gate_pre_ref[...])[0]
    rates = decay_ref[...]
    product, adjoint = scan_rows(shifted_back(rates, 1, 1.0), grad_states, shifted_back)
    local_ref[...] = adjoint
    product_ref[...] = product
    ends_ref[...] = jnp.concatenate(
        [
            rates[0:1] * product[0:1],
            rates[0:1] * adjoint[0:1],
        ],
        0,
    )


def gate_grads_kernel(
    position_ref,
    local_ref,
    product_ref,
    ends_ref,
    decay_ref,
    rgate_ref,
    igate_ref,
    conv_out_ref,
    states_ref,
    entry_ref,
    conv_in_ref,
    before_ref,
    weight_ref,
    rate_ref,
    grad_conv_ref,
    weight_grad_ref,
    sums_ref,
):
    position = position_ref[0]
    entry = jnp.zeros((1, local_ref.shape[1]), wide)
    for s in range(ends_ref.shape[0] - 1, 0, -1):
        earlier = ends_ref[s, 0:1, :] * entry + ends_ref[s, 1:2, :]
        entry = jnp.where(s > position, earlier, entry)
    adjoint = local_ref[...] + product_ref[...] * entry
    rates = decay_ref[...]
    rgate = rgate_ref[...]
    igate = igate_ref[...]
    conv_out = conv_out_ref[...]
    row = lax.broadcasted_iota(jnp.int32, rates.shape, 0)
    before = jnp.where(row == 0, entry_ref[0:1, :], pltpu.roll(states_ref[...], 1, 0))
    opening = opening_rows(rates.shape, position)
    log_rate = rate_ref[...] * rgate
    root = jnp.sqrt(one_minus_square(log_rate))
    scaling = jnp.where(opening, 1.0, root)
    grad_scaling = adjoint * igate * conv_out
    grad_log = adjoint * before * rates - jnp.where(
        opening, 0.0, grad_scaling * rates * rates / root
    )
    grad_rgate = grad_log * rate_ref[...] * rgate * (1.0 - rgate)
    grad_igate = adjoint * scaling * conv_out * igate * (1.0 - igate)
    grad_conv = adjoint * scaling * igate
    conv_low = conv_out.astype(low)
    sums = []
    for j, grad in enumerate((grad_rgate, grad_igate)):
        grad_low = grad.astype(low)
        sums.append(jnp.sum(grad_low.astype(wide), 0, keepdims=True))
        weight_grad_ref[j] = lax.dot_general(
            conv_low, grad_low, (((0,), (0,)), ((), ())), preferred_element_type=wide
        ).astype(low)
        grad_conv = grad_conv + lax.dot_general(
            grad_low, weight_ref[j, 0], (((1,), (1,)), ((), ())), preferred_element_type=wide
        )
    grad_conv_ref[...] = grad_conv
    sums.append(jnp.sum(grad_log * rgate, 0, keepdims=True))
    sums.append(jnp.sum(grad_conv, 0, keepdims=True))
    ext = jnp.concatenate([before_ref[...], conv_in_ref[...]], 0)
    for lag in range(4):
        moved = pltpu.roll(ext, lag, 0) if lag else ext
        sums.append(jnp.sum(grad_conv * moved[8:, :], 0, keepdims=True))
    sums_ref[...] = jnp.concatenate(sums, 0)


def branch_grads_kernel(
    grad_conv_ref, after_ref, taps_ref, gate_pre_ref, grad_mixed_ref, states_ref, out_ref, sums_ref
):
    grad_conv = grad_conv_ref[...]
    rows = grad_conv.shape[0]
    ext = jnp.concatenate([grad_conv, after_ref[...]], 0)
    total = taps_ref[0:1, :] * grad_conv
    for lag in range(1, taps_ref.shape[0]):
        moved = pltpu.roll(ext, rows + 8 - lag, 0)
        total = total + taps_ref[lag : lag + 1, :] * moved[:rows, :]
    slope = gelu_parts(gate_pre_ref[...])[1]
    grad_gate = slope * grad_mixed_ref[...] * states_ref[...]
    sums = []
    for j, grad in enumerate((grad_gate, total)):
        grad_low = grad.astype(low)
        out_ref[j] = grad_low
        sums.append(jnp.sum(grad_low.astype(wide), 0, keepdims=True))
    sums_ref[...] = jnp.concatenate(sums + [jnp.zeros((6, grad_conv.shape[1]), wide)], 0)


def by_heads(kernel, heads, width, operands, outs):
    def spec(shape):
        if len(shape) == 1:
            return in_smem
        if len(shape) == 4:
            return pl.BlockSpec((shape[0], 1, width, width), lambda h: (0, h, 0, 0))
        lead = shape[:-1]
        return pl.BlockSpec(lead + (width,), lambda h, rank=len(lead): (0,) * rank + (h,))

    return pl.pallas_call(
        kernel,
        grid=(heads,),
        out_shape=[jax.ShapeDtypeStruct(shape, dtype) for shape, dtype in outs],
        in_specs=[spec(value.shape) for value in operands],
        out_specs=[spec(shape) for shape, _ in outs],
        compiler_params=pltpu.CompilerParams(vmem_limit_bytes=48000000),
    )(*operands)


def joined_kernel(half, turned_ref, pre_ref, bias_ref, *out_refs):
    members, _, both = pre_ref.shape
    unit = both // (2 * half)
    bias = bias_ref[...]
    for k in range(half):
        for member in range(members):
            parts = [
                pre_ref[member, :, (j * half + k) * unit : (j * half + k + 1) * unit].astype(wide)
                for j in range(2)
            ]
            at = (k * members + member) * unit
            for j in range(2):
                value = jnp.where(turned_ref[0] == 1, parts[1 - j], parts[j])
                out_refs[j][:, at : at + unit] = value + bias[j : j + 1, at : at + unit]


def joined_columns(pre, bias, turned, half):
    shape = jax.ShapeDtypeStruct((pre.shape[1], bias.shape[1]), wide)
    return pl.pallas_call(
        functools.partial(joined_kernel, half),
        out_shape=[shape, shape],
        in_specs=[in_smem, in_vmem, in_vmem],
        out_specs=[in_vmem, in_vmem],
        compiler_params=pltpu.CompilerParams(vmem_limit_bytes=16 << 20),
        name="joined_columns",
    )(jnp.asarray(turned, jnp.int32).reshape(1), pre, bias)


def split_kernel(half, turned_ref, grads_ref, out_ref):
    members, _, both = out_ref.shape
    unit = both // (2 * half)
    for k in range(half):
        for member in range(members):
            at = (k * members + member) * unit
            parts = [grads_ref[j, :, at : at + unit] for j in range(2)]
            for j in range(2):
                value = jnp.where(turned_ref[0] == 1, parts[1 - j], parts[j])
                out_ref[member, :, (j * half + k) * unit : (j * half + k + 1) * unit] = value


def split_columns(grads, turned, half):
    _, rows, width = grads.shape
    return pl.pallas_call(
        functools.partial(split_kernel, half),
        out_shape=jax.ShapeDtypeStruct((block_size, rows, 2 * width // block_size), grads.dtype),
        in_specs=[in_smem, in_vmem],
        out_specs=in_vmem,
        compiler_params=pltpu.CompilerParams(vmem_limit_bytes=16 << 20),
        name="split_columns",
    )(jnp.asarray(turned, jnp.int32).reshape(1), grads)


def normed(values, scales):
    return values * lax.rsqrt(jnp.mean(values * values, -1, keepdims=True) + epsilon) * scales


def gated_unit(gate, up):
    return jax.nn.gelu(gate, approximate=True) * up


def times_rows(operand, weight):
    return lax.dot_general(
        operand, weight, (((1,), (1,)), ((), ())), preferred_element_type=wide
    )


def times(operand, weight):
    return jnp.dot(operand, weight, preferred_element_type=wide)


def row_sums(gradient, operand):
    return lax.dot_general(
        gradient, operand, (((0,), (0,)), ((), ())), preferred_element_type=wide
    )


def gain_sums(gradient, weight):
    return jnp.sum(gradient * weight.astype(wide), 0)


def member_columns(values):
    rows, width = values.shape
    count = lax.axis_size("g")
    split = values.reshape(rows, count, block_size, width // (count * block_size))
    return split.transpose(2, 0, 1, 3).reshape(block_size, rows, width // block_size)


def after(values, earlier):
    return lax.optimization_barrier((values, earlier))[0]


class Exchange:
    def __init__(self, values):
        self.values = values
        self.share = 0
        self.parts = []

    def next(self, share):
        tiles = self.values.shape[0] // 16
        start = tiles * self.share // 16 * 16
        self.share += share
        return self.values, start, tiles * self.share // 16 * 16 - start

    def shift(self, share, earlier):
        values, start, size = self.next(share)
        part = lax.slice_in_dim(values, start, start + size, axis=0)
        part = after(part, earlier)
        self.parts.append(group_shift(part, 1))

    def whole(self):
        return self.parts[0] if len(self.parts) == 1 else jnp.concatenate(self.parts, 0)


def sharing(paired, plan):
    if not paired:
        return ()
    return tuple(exchange.next(share) for exchange, share in plan)


def arrived(paired, plan, parts):
    if paired:
        for (exchange, _), part in zip(plan, parts):
            exchange.parts.append(part)


def body(
    inputs,
    gain_first,
    branch_weight,
    branch_bias,
    conv_weight,
    conv_bias,
    gate_weight,
    gate_bias,
    decay,
    out_weight,
    out_bias,
    gain_second,
    mlp_weight,
    down_weight,
    cotangent,
):
    source = inputs[0].astype(wide)
    rows, width = source.shape
    heads, head_width = gate_weight.shape[1:3]
    count = lax.axis_size("g")
    half = count // 2
    paired = count == 2
    turned = (lax.axis_index("g") == 1) if paired else False
    all_rows = block_size * rows
    position = (
        lax.axis_index("g") * 4 + lax.axis_index("b3") * 2 + lax.axis_index("b2")
    ).reshape(1)
    flat = (rows, width)
    small = (8, width)

    def in_turn(first, second):
        if not paired:
            return first, second
        return jnp.where(turned, second, first), jnp.where(turned, first, second)

    def turn_halves(values):
        if not paired:
            return values
        return jnp.where(turned, jnp.roll(values, width // 2, 1), values)

    def move(gathered, swapped, collective, plan):
        outs = block_move(gathered, swapped, collective, sharing(paired, plan))
        own = (gathered is not None) + len(swapped)
        arrived(paired, plan, outs[own:])
        return outs[0] if own == 1 else outs[:own]

    def scatter(products, collective, plan, extra=None):
        out, *parts = block_scatter(products, collective, sharing(paired, plan), extra)
        arrived(paired, plan, parts)
        return out

    def joined(values, exchange):
        if paired:
            return jnp.concatenate([values, exchange.whole()], 0)
        return group_gather(values).reshape(-1, values.shape[1])

    def total(own, exchange, sums):
        if paired:
            return own + exchange.whole().astype(wide)
        return group_sum(sums)

    down_rows, hidden_width = down_weight.shape
    unit = hidden_width // (half * block_size)
    down_split = (
        down_weight.reshape(down_rows, half, block_size, unit)
        .transpose(2, 0, 1, 3)
        .reshape(block_size, down_rows, half * unit)
    )
    mlp_trade = Exchange(mlp_weight)
    branch_trade = Exchange(branch_weight)
    out_rows = lax.all_gather(out_weight, places, axis=0, tiled=True)

    first_in = normed(source, gain_first).astype(low)
    first_all, down_own = move(
        first_in, (down_split,), 1, [(branch_trade, 16)]
    )
    down_own = down_own.reshape(block_size * down_rows, half * unit)
    down_trade = Exchange(down_own)
    first_all = first_all.reshape(all_rows, width)
    cot_in = after(turn_halves(cotangent[0]), first_all)
    cot_all = lax.all_gather(cot_in, cube, axis=0, tiled=True)
    grad_out = cotangent[0]
    branch_rows = joined(branch_weight, branch_trade)
    pre_part = times_rows(first_all, branch_rows).astype(low)
    pre_part = pre_part.reshape(block_size, rows, 2 * width // block_size)
    pre = move(None, (pre_part,), 2, [(mlp_trade, 7)])
    if paired:
        mlp_trade.shift(5, pre)
    gate_pre, conv_in = joined_columns(pre, branch_bias.reshape(2, width), turned, half)
    conv_before = rim_rows(conv_in[rows - 8 :], 1)

    rate = (-8.0 * jax.nn.softplus(decay))[None]
    conv_out, rgate, igate, decays, local, product, ends = by_heads(
        local_states_kernel,
        heads,
        head_width,
        (
            position,
            conv_in,
            conv_before,
            conv_weight,
            conv_bias[None],
            gate_weight,
            gate_bias,
            rate,
        ),
        [(flat, wide)] * 6 + [((2, width), wide)],
    )
    all_ends = seq_spread(ends, 3)
    if paired:
        mlp_trade.shift(4, all_ends)
    states, mixed, entry = by_heads(
        full_states_kernel,
        heads,
        head_width,
        (position, local, product, all_ends, gate_pre),
        [(flat, wide), (flat, low), (small, wide)],
    )
    middle = source + times_rows(mixed, out_rows) + out_bias

    second_in = normed(middle, gain_second).astype(low)
    second_all = move(second_in, (), 4, [(down_trade, 12)])
    if paired:
        down_trade.shift(4, second_all)
    second_all = second_all.reshape(all_rows, width)
    if paired:
        rows_a, rows_b = mlp_weight, mlp_trade.whole()
    else:
        mlp_rows = group_gather(mlp_weight)
        rows_a = mlp_rows[:half].reshape(-1, width)
        rows_b = mlp_rows[half:].reshape(-1, width)
    down_columns = joined(down_own, down_trade)
    pre_a = times_rows(second_all, rows_a)
    mlp_gate, mlp_up = in_turn(pre_a, times_rows(second_all, rows_b))
    mlp_hidden, gated_back = jax.vjp(gated_unit, mlp_gate, mlp_up)
    mlp_hidden = mlp_hidden.astype(low)
    grad_hidden = times(cot_all, down_columns)
    grad_a, grad_b = in_turn(*(grad.astype(low) for grad in gated_back(grad_hidden)))
    sum_b = row_sums(grad_b, second_all)
    sum_b_low = sum_b.astype(low)
    mlp_back = Exchange(sum_b_low)
    grad_second = scatter(
        [(grad_a, rows_a, False), (grad_b, rows_b, False)], 5, [(mlp_back, 8)]
    )
    down_sum = row_sums(cot_all, mlp_hidden)
    down_sums = down_sum.astype(low).reshape(count, block_size * down_rows, half * unit)
    down_back = Exchange(down_sums[1])
    down_left = after(mlp_hidden, grad_second)
    down_full = scatter([(down_left, down_columns, True)], 6, [(mlp_back, 8)])
    output = (middle + turn_halves(down_full)).astype(low)[None]
    if paired:
        down_back.shift(5, down_full)

    _, second_back = jax.vjp(lambda values: normed(values, gain_second), middle)
    grad_middle = grad_out.astype(wide) + second_back(grad_second)[0]
    grad_branch = grad_middle.astype(low)
    out_bias_term = jnp.sum(grad_branch.astype(wide), 0)
    grad_mixed = times(grad_branch, out_rows)

    adjoint, tail, adjoint_ends = by_heads(
        local_adjoint_kernel,
        heads,
        head_width,
        (grad_mixed, gate_pre, decays),
        [(flat, wide), (flat, wide), ((2, width), wide)],
    )
    all_adjoint_ends = seq_spread(adjoint_ends, 9)
    mixed_all = lax.all_gather(after(mixed, all_adjoint_ends), cube, axis=0, tiled=True)
    if paired:
        down_back.shift(9, all_adjoint_ends)
    grad_conv, gate_weight_term, gate_sums = by_heads(
        gate_grads_kernel,
        heads,
        head_width,
        (
            position,
            adjoint,
            tail,
            all_adjoint_ends,
            decays,
            rgate,
            igate,
            conv_out,
            states,
            entry,
            conv_in,
            conv_before,
            gate_weight,
            rate,
        ),
        [(flat, wide), ((2, head_width, width), low), (small, wide)],
    )
    conv_after = rim_rows(grad_conv[:8], -1)
    pre_grads, pre_sums = by_heads(
        branch_grads_kernel,
        heads,
        head_width,
        (grad_conv, conv_after, conv_weight, gate_pre, grad_mixed, states),
        [((2, rows, width), low), (small, wide)],
    )

    columns = split_columns(pre_grads, turned, half)
    pre_all, branch_all = move(None, (columns, member_columns(grad_branch)), 10, [])
    branch_all = branch_all.reshape(all_rows, -1)
    sum_a = row_sums(grad_a, second_all)
    mlp_low = jnp.concatenate([sum_a.astype(low), sum_b_low], 0).reshape(count, -1, width)
    gain_second_term = gain_sums(sum_a, rows_a) + gain_sums(sum_b, rows_b)
    out_sum = row_sums(branch_all, mixed_all).reshape(count, -1, width)
    out_sums = out_sum.astype(low)
    own_out, other_out = in_turn(out_sum[0], out_sum[1])
    out_back = Exchange(other_out.astype(low))
    if paired:
        down_back.shift(2, pre_all)
    pre_all = pre_all.reshape(all_rows, -1)
    branch_sum = row_sums(pre_all, first_all)
    branch_sums = branch_sum.astype(low).reshape(count, -1, width)
    branch_back = Exchange(branch_sums[1])
    gain_first_term = gain_sums(branch_sum, branch_rows)

    tops = jnp.stack([out_bias_term, gain_first_term, gain_second_term], 0)
    vectors = jnp.concatenate([gate_sums, pre_sums[:2], tops, jnp.zeros((3, width), wide)], 0)
    vectors = vectors.astype(low)
    gate_terms = gate_weight_term.reshape(block_size, -1, width)
    gate_unit = gate_terms.shape[1]
    shared_part = jnp.concatenate(
        [
            gate_terms,
            vectors[:, None, :],
            jnp.zeros((block_size, 15, width), low),
        ],
        1,
    )
    scattered = scatter(
        [(pre_all, branch_rows, False)], 11, [(branch_back, 10), (out_back, 16)], shared_part
    )
    grad_first = scattered[:rows]
    _, first_back = jax.vjp(lambda values: normed(values, gain_first), source)
    input_grad = (grad_middle + first_back(grad_first)[0])[None]
    shared = group_total(scattered[rows:]).astype(low)
    mlp_grad = total(sum_a, mlp_back, mlp_low)

    if paired:
        down_total = down_sum[: block_size * down_rows] + down_back.whole().astype(wide)
    else:
        down_total = group_sum(down_sums)
    down_total = down_total.astype(low).reshape(block_size, down_rows, half * unit)
    shared_all, down_total = move(shared, (down_total,), 7, [(branch_back, 6)])
    down_grad = (
        down_total.reshape(block_size, down_rows, half, unit)
        .transpose(1, 2, 0, 3)
        .reshape(down_rows, hidden_width)
        .astype(wide)
    )
    gate_sum = shared_all[:, :gate_unit].reshape(2, head_width, width)
    gate_weight_grad = jnp.stack(
        [gate_sum[:, :, h * head_width : (h + 1) * head_width] for h in range(heads)], 1
    ).astype(wide)
    sums = shared_all[:, gate_unit].astype(wide)
    branch_grad = total(branch_sum[: branch_weight.shape[0]], branch_back, branch_sums)
    out_grad = total(own_out, out_back, out_sums)
    return (
        output,
        input_grad,
        sums[11] / gain_first,
        branch_grad,
        sums[8:10].reshape(-1),
        sums[4:8],
        sums[3],
        gate_weight_grad,
        sums[:2],
        sums[2] * (-8.0 * jax.nn.sigmoid(decay)),
        out_grad,
        sums[10],
        sums[12] / gain_second,
        mlp_grad,
        down_grad,
    )


def solution(mesh):
    count = mesh.devices.size // block_size
    blocks = Mesh(mesh.devices.reshape((count,) + (2,) * len(cube)), places)
    tokens = P(fsdp_axes, seq_axes, None)
    owned = P(places, None)
    return jax.shard_map(
        body,
        mesh=blocks,
        in_specs=(
            tokens,
            P(),
            owned,
            P(),
            P(),
            P(),
            P(),
            P(),
            P(),
            owned,
            P(),
            P(),
            owned,
            owned,
            tokens,
        ),
        out_specs=(
            tokens,
            tokens,
            P(),
            owned,
            P(),
            P(),
            P(),
            P(),
            P(),
            P(),
            owned,
            P(),
            P(),
            owned,
            owned,
        ),
        check_vma=False,
    )
```

```python
import functools

import jax
import jax.numpy as jnp
from jax import lax
from jax.experimental import pallas as pl
from jax.experimental.pallas import tpu as pltpu
from jax.sharding import Mesh
from jax.sharding import PartitionSpec as P

epsilon = 1e-06
low = jnp.bfloat16
wide = jnp.float32

cube = ("b3", "b2", "b1", "b0")
block_size = 16
places = ("g",) + cube
seq_axes = ("g", "b3", "b2")
fsdp_axes = ("b1", "b0")
first_orders = (("b3", "b1", "b2"), ("b3", "b2", "b1"))
even_orders = (("b1", "b3", "b2"), ("b2", "b3", "b1"))

anywhere = pl.BlockSpec(memory_space=pl.ANY)
in_vmem = pl.BlockSpec(memory_space=pltpu.VMEM)
in_smem = pl.BlockSpec(memory_space=pltpu.SMEM)
whole_vmem = 67000000


def bit_of(axis):
    return 1 << (len(cube) - 1 - cube.index(axis))


def slot_at(mask):
    slot = 0
    for axis in cube:
        here = lax.axis_index(axis)
        slot = slot * 2 + (1 - here if mask & bit_of(axis) else here)
    return slot


def device_at(mask):
    return {axis: 1 - lax.axis_index(axis) for axis in cube if mask & bit_of(axis)}


def greet(masks, paired):
    barrier = pltpu.get_barrier_semaphore()
    targets = [device_at(mask) for mask in masks] + [other_block()] * paired
    for target in targets:
        pl.semaphore_signal(
            barrier, inc=1, device_id=target, device_id_type=pl.DeviceIdType.MESH
        )
    pl.semaphore_wait(barrier, len(targets))


def other_block():
    return {"g": 1 - lax.axis_index("g")}


class Ride:
    def __init__(self, riders):
        self.arrays = [array for array, _, _ in riders]
        self.ranges = [(start, size) for _, start, size in riders]
        self.chunks = []
        for number, (array, start, size) in enumerate(riders):
            step = 16 if array.shape[1] > 4096 else (48 if array.shape[1] > 1024 else 160)
            for begin in range(0, size, step):
                self.chunks.append((number, start + begin, begin, min(step, size - begin)))

    def shapes(self):
        return [
            jax.ShapeDtypeStruct((size,) + array.shape[1:], array.dtype)
            for array, (_, size) in zip(self.arrays, self.ranges)
        ]

    def semaphores(self):
        count = max(1, len(self.chunks))
        return [pltpu.SemaphoreType.DMA((count,)), pltpu.SemaphoreType.DMA((count,))]

    def enter(self, inputs, outputs, send_sem, recv_sem):
        self.copies = [
            pltpu.make_async_remote_copy(
                src_ref=inputs[number].at[pl.ds(begin, size)],
                dst_ref=outputs[number].at[pl.ds(start, size)],
                send_sem=send_sem.at[chunk],
                recv_sem=recv_sem.at[chunk],
                device_id=other_block(),
                device_id_type=pl.DeviceIdType.MESH,
            )
            for chunk, (number, begin, start, size) in enumerate(self.chunks)
        ]
        self.started = 0

    def start(self, share):
        until = -(-len(self.copies) * share[0] // share[1])
        for copy in self.copies[self.started : until]:
            copy.start()
        self.started = max(self.started, until)

    def finish(self):
        self.start((1, 1))
        for copy in self.copies:
            copy.wait()


def split_rows(rows, orders):
    tiles = rows // 16
    pieces = []
    start = 0
    for number, order in enumerate(orders):
        size = (tiles + len(orders) - 1 - number) // len(orders) * 16
        if size:
            pieces.append((order, start, size))
        start += size
    return pieces


def hop_orders(riders):
    return first_orders + even_orders if riders else even_orders


def remote_params(collective, held):
    return pltpu.CompilerParams(
        collective_id=collective,
        has_side_effects=True,
        vmem_limit_bytes=min(whole_vmem, held + (2 << 20)),
    )


def bytes_of(*values):
    return sum(value.size * value.dtype.itemsize for value in values)


def move_kernel(pieces, swap_count, ride, *refs):
    refs = list(refs)

    def take(count):
        taken = refs[:count]
        del refs[:count]
        return taken

    gathers = 1 if pieces else 0
    count = len(ride.arrays)
    sources, swaps, riders = take(gathers), take(swap_count), take(count)
    targets, swapped, arrivals = take(gathers), take(swap_count), take(count)
    send_sem, recv_sem, local_sem, swap_send, swap_recv, ride_send, ride_recv = refs
    neighbours = [bit_of(axis) for axis in cube]
    greet(list(range(1, block_size)) if swap_count else neighbours, count > 0)
    ride.enter(riders, arrivals, ride_send, ride_recv)
    sent = []
    here = slot_at(0)
    locals_ = []

    def push(part, start, size, mask, axis):
        slot = slot_at(mask)
        source = (sources[0] if mask == 0 else targets[0].at[slot]).at[pl.ds(start, size)]
        copy = pltpu.make_async_remote_copy(
            src_ref=source,
            dst_ref=targets[0].at[slot].at[pl.ds(start, size)],
            send_sem=send_sem.at[len(sent)],
            recv_sem=recv_sem.at[part, mask ^ bit_of(axis)],
            device_id=device_at(bit_of(axis)),
            device_id_type=pl.DeviceIdType.MESH,
        )
        copy.start()
        sent.append(copy)

    def arrive(part, start, size, mask):
        target = targets[0].at[slot_at(mask)].at[pl.ds(start, size)]
        pltpu.make_async_copy(target, target, recv_sem.at[part, mask]).wait()

    def forward(stage):
        for part, (order, start, size) in enumerate(pieces):
            order = order + ("b0",)
            masks = [0]
            if stage > 0:
                for axis in order[: stage - 1]:
                    masks = masks + [mask | bit_of(axis) for mask in masks]
                masks = [mask | bit_of(order[stage - 1]) for mask in masks]
            for mask in masks:
                if mask:
                    arrive(part, start, size, mask)
                for axis in order[stage:]:
                    push(part, start, size, mask, axis)

    forward(0)
    swap_copies = []
    for mask in (15, 14, 13, 11, 7, 12, 10, 6, 9, 5, 3, 8, 4, 2, 1):
        for number in range(swap_count):
            copy = pltpu.make_async_remote_copy(
                src_ref=swaps[number].at[slot_at(mask)],
                dst_ref=swapped[number].at[here],
                send_sem=swap_send.at[number, mask],
                recv_sem=swap_recv.at[number, mask],
                device_id=device_at(mask),
                device_id_type=pl.DeviceIdType.MESH,
            )
            copy.start()
            swap_copies.append(copy)
    ride.start((1, 1))
    for number in range(gathers):
        locals_.append((sources[number], targets[number].at[here]))
    for number in range(swap_count):
        locals_.append((swaps[number].at[here], swapped[number].at[here]))
    locals_ = [
        pltpu.make_async_copy(source, target, local_sem.at[number])
        for number, (source, target) in enumerate(locals_)
    ]
    for copy in locals_:
        copy.start()
    for stage in (1, 2, 3):
        forward(stage)
    for part, (_, start, size) in enumerate(pieces):
        for mask in range(block_size):
            if mask & bit_of("b0"):
                arrive(part, start, size, mask)
    for number in range(swap_count):
        for mask in range(1, block_size):
            target = swapped[number].at[slot_at(mask)]
            pltpu.make_async_copy(target, target, swap_recv.at[number, mask]).wait()
    for copy in sent + swap_copies:
        copy.wait_send()
    for copy in locals_:
        copy.wait()
    ride.finish()


def block_move(gathered, swapped, collective, riders=()):
    pieces = []
    shapes = []
    gathers = [] if gathered is None else [gathered]
    for values in gathers:
        pieces = split_rows(values.shape[0], hop_orders(riders))
        shapes.append(jax.ShapeDtypeStruct((block_size,) + values.shape, values.dtype))
    for values in swapped:
        shapes.append(jax.ShapeDtypeStruct(values.shape, values.dtype))
    ride = Ride(riders)
    swaps = max(1, len(swapped))
    moved = len(gathers) * [anywhere] + len(swapped) * [in_vmem] + len(riders) * [anywhere]
    return pl.pallas_call(
        functools.partial(move_kernel, pieces, len(swapped), ride),
        out_shape=shapes + ride.shapes(),
        in_specs=len(gathers) * [in_vmem] + moved[len(gathers) :],
        out_specs=moved,
        scratch_shapes=[
            pltpu.SemaphoreType.DMA((max(1, 15 * len(pieces)),)),
            pltpu.SemaphoreType.DMA((max(1, len(pieces)), block_size)),
            pltpu.SemaphoreType.DMA((1 + swaps,)),
            pltpu.SemaphoreType.DMA((swaps, block_size)),
            pltpu.SemaphoreType.DMA((swaps, block_size)),
        ]
        + ride.semaphores(),
        compiler_params=remote_params(
            collective, 2 * bytes_of(*gathers) + 4 * bytes_of(*swapped)
        ),
        name="block_move",
    )(*gathers, *swapped, *ride.arrays)


def scatter_kernel(pieces, product_rows, transposed, extra_count, ride, *refs):
    refs = list(refs)

    def take(count):
        taken = refs[:count]
        del refs[:count]
        return taken

    products = len(transposed)
    count = len(ride.arrays)
    left_refs, right_refs, extras, riders = (
        take(products),
        take(products),
        take(extra_count),
        take(count),
    )
    (out_ref,), arrivals = take(1), take(count)
    left_rows = take(products)
    held, away, send_sem, recv_sem, left_sem, load_sem, ride_send, ride_recv = refs
    core = bit_of("b0")
    members = 2 * product_rows
    order_count = [sum(mask >> bit & 1 for bit in range(len(cube))) for mask in range(block_size)]
    steps = sorted(
        (mask for mask in range(block_size) if not mask & core),
        key=lambda mask: (-order_count[mask], -mask),
    )
    here = lax.axis_index("b0")

    def left_copy(number, step):
        pair = slot_at(steps[step]) // 2
        rows = pl.ds(pl.multiple_of(pair * members, members), members)
        return pltpu.make_async_copy(
            left_refs[number].at[rows], left_rows[number].at[step], left_sem.at[number, step]
        )

    for step in range(8):
        for number in range(products):
            left_copy(number, step).start()
    greet([bit_of(axis) for axis in cube], count > 0)
    ride.enter(riders, arrivals, ride_send, ride_recv)
    sent = []

    def slot_of(order, hop, mask):
        clear = [bit_of(axis) for axis in order[:hop]] + [core]
        masks = [m for m in range(block_size) if not any(m & bit for bit in clear)]
        return (0, 8, 12, 14)[hop] + masks.index(mask)

    def push(source, number, slot, axis):
        _, _, _, start, size = pieces[number]
        copy = pltpu.make_async_remote_copy(
            src_ref=source,
            dst_ref=away.at[slot].at[pl.ds(start, size)],
            send_sem=send_sem.at[len(sent)],
            recv_sem=recv_sem.at[number, slot],
            device_id=device_at(bit_of(axis)),
            device_id_type=pl.DeviceIdType.MESH,
        )
        copy.start()
        sent.append(copy)

    def arrive(number, slot):
        _, _, _, start, size = pieces[number]
        target = away.at[slot].at[pl.ds(start, size)]
        pltpu.make_async_copy(target, target, recv_sem.at[number, slot]).wait()

    tile = 512

    def work_out(step):
        for number in range(products):
            left_copy(number, step).wait()

        def columns(i, carry):
            at = pl.ds(pl.multiple_of(i * tile, tile), tile)
            total = None
            for number in range(products):
                left = left_rows[number][step]
                if transposed[number]:
                    term = lax.dot_general(
                        left,
                        right_refs[number][at, :],
                        (((1,), (1,)), ((), ())),
                        preferred_element_type=wide,
                    )
                else:
                    term = jnp.dot(left, right_refs[number][:, at], preferred_element_type=wide)
                total = term if total is None else total + term
            total = total.astype(low)
            held[step, 0, pl.ds(0, product_rows), at] = total[:product_rows]
            held[step, 1, pl.ds(0, product_rows), at] = total[product_rows:]
            return carry

        lax.fori_loop(0, out_ref.shape[1] // tile, columns, 0)
        for number, (order, extra, begin, start, size) in enumerate(pieces):
            rows = pl.ds(begin, size)
            if extra:
                source = extras[0].at[slot_at(steps[step] | core)].at[rows]
            else:
                source = held.at[step, 1 - here].at[rows]
            push(source, number, slot_of(order, 0, steps[step]), "b0")

    loads = {}
    for step in range(8):
        for number, (order, extra, begin, start, size) in enumerate(pieces):
            if extra:
                loads[number, step] = pltpu.make_async_copy(
                    extras[0].at[slot_at(steps[step])].at[pl.ds(begin, size)],
                    held.at[step, here].at[pl.ds(start, size)],
                    load_sem.at[number, step],
                )
                loads[number, step].start()

    def pass_on(step):
        mask = steps[step]
        for number, (order, extra, begin, start, size) in enumerate(pieces):
            bits = [bit_of(axis) for axis in order]
            if extra:
                loads[number, step].wait()
            slots = [slot_of(order, 0, mask)]
            target = None
            for hop, bit in enumerate(bits):
                if mask & bit:
                    target = hop
                    break
                slots.append(slot_of(order, hop + 1, mask))
            for slot in slots:
                arrive(number, slot)

            def add_tile(i, carry, start=start, slots=slots, target=target):
                at = pl.ds(pl.multiple_of(start + i * 16, 16), 16)
                total = held[step, here, at, :].astype(wide)
                for slot in slots:
                    total = total + away[slot, at, :].astype(wide)
                if target is None:
                    out_ref[at, :] = total.astype(out_ref.dtype)
                else:
                    held[step, here, at, :] = total.astype(low)
                return carry

            lax.fori_loop(0, size // 16, add_tile, 0)
            if target is not None:
                push(
                    held.at[step, here].at[pl.ds(start, size)],
                    number,
                    slot_of(order, target + 1, mask ^ bits[target]),
                    order[target],
                )

    for step in range(9):
        if step < 8:
            work_out(step)
        if step == 0:
            ride.start((1, 1))
        if step > 0:
            pass_on(step - 1)
    for copy in sent:
        copy.wait_send()
    ride.finish()


def block_scatter(products, collective, riders=(), extra=None):
    ride = Ride(riders)
    lefts = [left for left, _, _ in products]
    rights = [right for _, right, _ in products]
    transposed = [flag for _, _, flag in products]
    product_rows = lefts[0].shape[0] // block_size
    width = rights[0].shape[0] if transposed[0] else rights[0].shape[1]
    extras = [] if extra is None else [extra]
    orders = [order[::-1] for order in hop_orders(riders)]
    pieces = [
        (order, 0, start, start, size) for order, start, size in split_rows(product_rows, orders)
    ]
    rows = product_rows
    for values in extras:
        for order, start, size in split_rows(values.shape[1], orders):
            pieces.append((order, 1, start, rows + start, size))
        rows += values.shape[1]
    padded = [-(-left.shape[1] // 128) * 128 for left in lefts]
    held_bytes = (
        (16 + 15) * rows * width * 2
        + 2 * rows * width * 4
        + sum(2 * left.shape[0] * size for left, size in zip(lefts, padded))
        + 2 * sum(2 * size * width for size in padded)
        + (8 << 20)
    )
    return pl.pallas_call(
        functools.partial(
            scatter_kernel, pieces, product_rows, transposed, len(extras), ride
        ),
        out_shape=[jax.ShapeDtypeStruct((rows, width), wide)] + ride.shapes(),
        in_specs=[anywhere] * len(lefts)
        + [in_vmem] * len(rights)
        + [anywhere] * (len(extras) + len(riders)),
        out_specs=[in_vmem] + [anywhere] * len(riders),
        scratch_shapes=[pltpu.VMEM((8, 2 * product_rows, left.shape[1]), low) for left in lefts]
        + [
            pltpu.VMEM((8, 2, rows, width), low),
            pltpu.VMEM((15, rows, width), low),
            pltpu.SemaphoreType.DMA((15 * len(pieces),)),
            pltpu.SemaphoreType.DMA((len(pieces), 15)),
            pltpu.SemaphoreType.DMA((len(lefts), 8)),
            pltpu.SemaphoreType.DMA((len(pieces), 8)),
        ]
        + ride.semaphores(),
        compiler_params=remote_params(collective, held_bytes),
        name="block_scatter",
    )(*lefts, *rights, *extras, *ride.arrays)


def group_shift(values, distance):
    count = lax.axis_size("g")
    return lax.ppermute(values, "g", [(i, (i + distance) % count) for i in range(count)])


def group_gather(values):
    return lax.all_gather(values, "g", axis=0)


def group_sum(partials):
    return lax.psum_scatter(partials.astype(low), "g", scatter_dimension=0).astype(wide)


def group_total(values):
    count = lax.axis_size("g")
    total = values
    for distance in range(1, count):
        total = total + group_shift(values.astype(low), distance).astype(wide)
    return total


def spread_kernel(group_count, x_ref, out_ref, send_sem, recv_sem, local_sem):
    here_g, here_3, here_2 = (lax.axis_index(axis) for axis in seq_axes)
    peers = []
    for step in range(group_count):
        for mask in range(4):
            if step or mask:
                peers.append((step, mask))

    def place(step, mask):
        return (
            lax.rem(here_g + step, group_count),
            1 - here_3 if mask & 2 else here_3,
            1 - here_2 if mask & 1 else here_2,
        )

    barrier = pltpu.get_barrier_semaphore()
    for step, mask in peers:
        pl.semaphore_signal(
            barrier,
            inc=1,
            device_id=dict(zip(seq_axes, place(step, mask))),
            device_id_type=pl.DeviceIdType.MESH,
        )
    pl.semaphore_wait(barrier, len(peers))
    mine = here_g * 4 + here_3 * 2 + here_2
    sent = []
    for number, (step, mask) in enumerate(peers):
        copy = pltpu.make_async_remote_copy(
            src_ref=x_ref,
            dst_ref=out_ref.at[mine],
            send_sem=send_sem.at[number],
            recv_sem=recv_sem.at[number],
            device_id=dict(zip(seq_axes, place(step, mask))),
            device_id_type=pl.DeviceIdType.MESH,
        )
        copy.start()
        sent.append(copy)
    own = pltpu.make_async_copy(x_ref, out_ref.at[mine], local_sem)
    own.start()
    for number, (step, mask) in enumerate(peers):
        from_g, from_3, from_2 = place(group_count - step, mask)
        target = out_ref.at[from_g * 4 + from_3 * 2 + from_2]
        pltpu.make_async_copy(target, target, recv_sem.at[number]).wait()
    for copy in sent:
        copy.wait_send()
    own.wait()


def seq_spread(values, collective):
    group_count = lax.axis_size("g")
    count = 4 * group_count
    return pl.pallas_call(
        functools.partial(spread_kernel, group_count),
        out_shape=jax.ShapeDtypeStruct((count,) + values.shape, values.dtype),
        in_specs=[in_vmem],
        out_specs=in_vmem,
        scratch_shapes=[
            pltpu.SemaphoreType.DMA((count,)),
            pltpu.SemaphoreType.DMA((count,)),
            pltpu.SemaphoreType.DMA,
        ],
        compiler_params=remote_params(collective, 2 * (count + 1) * 8 * bytes_of(values)),
        name="seq_spread",
    )(values)


def rim_rows(values, offset):
    count = 4 * lax.axis_size("g")
    route = [(i - offset, i) for i in range(count) if 0 <= i - offset < count]
    return lax.ppermute(values, seq_axes, route)


def gelu_parts(v):
    inner = 0.7978845608028654 * (v + 0.044715 * v * v * v)
    t = jnp.tanh(inner)
    value = 0.5 * v * (1.0 + t)
    slope = 0.5 * (1.0 + t) + 0.5 * v * (1.0 - t * t) * 0.7978845608028654 * (
        1.0 + 0.134145 * v * v
    )
    return value, slope


def shifted(values, distance, fill):
    rows = values.shape[0]
    if distance % 8 == 0:
        head = jnp.full((distance,) + values.shape[1:], fill, values.dtype)
        return jnp.concatenate([head, values[: rows - distance]], 0)
    row = lax.broadcasted_iota(jnp.int32, values.shape, 0)
    return jnp.where(row >= distance, pltpu.roll(values, distance, 0), fill)


def shifted_back(values, distance, fill):
    rows = values.shape[0]
    if distance % 8 == 0:
        tail = jnp.full((distance,) + values.shape[1:], fill, values.dtype)
        return jnp.concatenate([values[distance:], tail], 0)
    row = lax.broadcasted_iota(jnp.int32, values.shape, 0)
    return jnp.where(row < rows - distance, pltpu.roll(values, rows - distance, 0), fill)


def scan_rows(rates, terms, shift):
    distance = 1
    while distance < rates.shape[0]:
        terms = terms + rates * shift(terms, distance, 0.0)
        rates = rates * shift(rates, distance, 1.0)
        distance *= 2
    return rates, terms


def one_minus_square(log_rate):
    x = 2.0 * log_rate
    series = 1.0
    for n in (9, 8, 7, 6, 5, 4, 3, 2):
        series = 1.0 + x * (1.0 / n) * series
    return jnp.where(x > -0.5, -x * series, 1.0 - jnp.exp(x))


def lagged_sum(ext, weights, start):
    total = start
    for lag in range(weights.shape[0]):
        moved = pltpu.roll(ext, lag, 0) if lag else ext
        total = total + weights[lag : lag + 1, :] * moved[8:, :]
    return total


def opening_rows(shape, position):
    return (lax.broadcasted_iota(jnp.int32, shape, 0) == 0) & (position == 0)


def conv_and_gates(conv_in_ref, before_ref, taps_ref, bias_ref, weight_ref, gate_bias_ref):
    ext = jnp.concatenate([before_ref[...], conv_in_ref[...]], 0)
    conv_out = lagged_sum(ext, taps_ref[...], bias_ref[...])
    conv_low = conv_out.astype(low)
    gates = [
        jax.nn.sigmoid(
            jnp.dot(conv_low, weight_ref[j, 0], preferred_element_type=wide)
            + gate_bias_ref[j : j + 1, :]
        )
        for j in range(2)
    ]
    return ext, conv_out, conv_low, gates


def local_states_kernel(
    position_ref,
    conv_in_ref,
    before_ref,
    taps_ref,
    bias_ref,
    weight_ref,
    gate_bias_ref,
    rate_ref,
    decay_ref,
    local_ref,
    product_ref,
    ends_ref,
):
    _, conv_out, _, gates = conv_and_gates(
        conv_in_ref, before_ref, taps_ref, bias_ref, weight_ref, gate_bias_ref
    )
    log_rate = rate_ref[...] * gates[0]
    rates = jnp.exp(log_rate)
    scaling = jnp.where(
        opening_rows(rates.shape, position_ref[0]), 1.0, jnp.sqrt(one_minus_square(log_rate))
    )
    product, states = scan_rows(rates, scaling * gates[1] * conv_out, shifted)
    decay_ref[...] = rates
    local_ref[...] = states
    product_ref[...] = product
    rows = rates.shape[0]
    ends_ref[...] = jnp.concatenate(
        [
            product[rows - 1 :],
            states[rows - 1 :],
        ],
        0,
    )


def full_states_kernel(
    position_ref, local_ref, product_ref, ends_ref, gate_pre_ref, states_ref, mixed_ref, entry_ref
):
    entry = jnp.zeros((1, local_ref.shape[1]), wide)
    for s in range(ends_ref.shape[0]):
        later = ends_ref[s, 0:1, :] * entry + ends_ref[s, 1:2, :]
        entry = jnp.where(s < position_ref[0], later, entry)
    states = local_ref[...] + product_ref[...] * entry
    states_ref[...] = states
    mixed_ref[...] = (states * gelu_parts(gate_pre_ref[...])[0]).astype(low)
    entry_ref[...] = jnp.broadcast_to(entry, entry_ref.shape)


def local_adjoint_kernel(
    grad_mixed_ref, gate_pre_ref, decay_ref, local_ref, product_ref, ends_ref
):
    grad_states = grad_mixed_ref[...] * gelu_parts(gate_pre_ref[...])[0]
    rates = decay_ref[...]
    product, adjoint = scan_rows(shifted_back(rates, 1, 1.0), grad_states, shifted_back)
    local_ref[...] = adjoint
    product_ref[...] = product
    ends_ref[...] = jnp.concatenate(
        [
            rates[0:1] * product[0:1],
            rates[0:1] * adjoint[0:1],
        ],
        0,
    )


def gate_grads_kernel(
    position_ref,
    local_ref,
    product_ref,
    ends_ref,
    decay_ref,
    states_ref,
    entry_ref,
    conv_in_ref,
    before_ref,
    taps_ref,
    bias_ref,
    weight_ref,
    gate_bias_ref,
    rate_ref,
    grad_conv_ref,
    weight_grad_ref,
    sums_ref,
):
    position = position_ref[0]
    entry = jnp.zeros((1, local_ref.shape[1]), wide)
    for s in range(ends_ref.shape[0] - 1, 0, -1):
        earlier = ends_ref[s, 0:1, :] * entry + ends_ref[s, 1:2, :]
        entry = jnp.where(s > position, earlier, entry)
    adjoint = local_ref[...] + product_ref[...] * entry
    rates = decay_ref[...]
    ext, conv_out, conv_low, (rgate, igate) = conv_and_gates(
        conv_in_ref, before_ref, taps_ref, bias_ref, weight_ref, gate_bias_ref
    )
    row = lax.broadcasted_iota(jnp.int32, rates.shape, 0)
    before = jnp.where(row == 0, entry_ref[0:1, :], pltpu.roll(states_ref[...], 1, 0))
    opening = opening_rows(rates.shape, position)
    log_rate = rate_ref[...] * rgate
    root = jnp.sqrt(one_minus_square(log_rate))
    scaling = jnp.where(opening, 1.0, root)
    grad_scaling = adjoint * igate * conv_out
    grad_log = adjoint * before * rates - jnp.where(
        opening, 0.0, grad_scaling * rates * rates / root
    )
    grad_rgate = grad_log * rate_ref[...] * rgate * (1.0 - rgate)
    grad_igate = adjoint * scaling * conv_out * igate * (1.0 - igate)
    grad_conv = adjoint * scaling * igate
    sums = []
    for j, grad in enumerate((grad_rgate, grad_igate)):
        grad_low = grad.astype(low)
        sums.append(jnp.sum(grad_low.astype(wide), 0, keepdims=True))
        weight_grad_ref[j] = lax.dot_general(
            conv_low, grad_low, (((0,), (0,)), ((), ())), preferred_element_type=wide
        ).astype(low)
        grad_conv = grad_conv + lax.dot_general(
            grad_low, weight_ref[j, 0], (((1,), (1,)), ((), ())), preferred_element_type=wide
        )
    grad_conv_ref[...] = grad_conv
    sums.append(jnp.sum(grad_log * rgate, 0, keepdims=True))
    sums.append(jnp.sum(grad_conv, 0, keepdims=True))
    for lag in range(4):
        moved = pltpu.roll(ext, lag, 0) if lag else ext
        sums.append(jnp.sum(grad_conv * moved[8:, :], 0, keepdims=True))
    sums_ref[...] = jnp.concatenate(sums, 0)


def branch_grads_kernel(
    grad_conv_ref, after_ref, taps_ref, gate_pre_ref, grad_mixed_ref, states_ref, out_ref, sums_ref
):
    grad_conv = grad_conv_ref[...]
    rows = grad_conv.shape[0]
    ext = jnp.concatenate([grad_conv, after_ref[...]], 0)
    total = taps_ref[0:1, :] * grad_conv
    for lag in range(1, taps_ref.shape[0]):
        moved = pltpu.roll(ext, rows + 8 - lag, 0)
        total = total + taps_ref[lag : lag + 1, :] * moved[:rows, :]
    slope = gelu_parts(gate_pre_ref[...])[1]
    grad_gate = slope * grad_mixed_ref[...] * states_ref[...]
    sums = []
    for j, grad in enumerate((grad_gate, total)):
        grad_low = grad.astype(low)
        out_ref[j] = grad_low
        sums.append(jnp.sum(grad_low.astype(wide), 0, keepdims=True))
    sums_ref[...] = jnp.concatenate(sums + [jnp.zeros((6, grad_conv.shape[1]), wide)], 0)


def by_heads(kernel, heads, width, operands, outs):
    def spec(shape):
        if len(shape) == 1:
            return in_smem
        if len(shape) == 4:
            return pl.BlockSpec((shape[0], 1, width, width), lambda h: (0, h, 0, 0))
        lead = shape[:-1]
        return pl.BlockSpec(lead + (width,), lambda h, rank=len(lead): (0,) * rank + (h,))

    return pl.pallas_call(
        kernel,
        grid=(heads,),
        out_shape=[jax.ShapeDtypeStruct(shape, dtype) for shape, dtype in outs],
        in_specs=[spec(value.shape) for value in operands],
        out_specs=[spec(shape) for shape, _ in outs],
        compiler_params=pltpu.CompilerParams(vmem_limit_bytes=12 << 20),
    )(*operands)


def joined_kernel(half, turned_ref, pre_ref, bias_ref, *out_refs):
    members, _, both = pre_ref.shape
    unit = both // (2 * half)
    bias = bias_ref[...]
    for k in range(half):
        for member in range(members):
            parts = [
                pre_ref[member, :, (j * half + k) * unit : (j * half + k + 1) * unit].astype(wide)
                for j in range(2)
            ]
            at = (k * members + member) * unit
            for j in range(2):
                value = jnp.where(turned_ref[0] == 1, parts[1 - j], parts[j])
                out_refs[j][:, at : at + unit] = value + bias[j : j + 1, at : at + unit]


def joined_columns(pre, bias, turned, half):
    shape = jax.ShapeDtypeStruct((pre.shape[1], bias.shape[1]), wide)
    return pl.pallas_call(
        functools.partial(joined_kernel, half),
        out_shape=[shape, shape],
        in_specs=[in_smem, in_vmem, in_vmem],
        out_specs=[in_vmem, in_vmem],
        compiler_params=pltpu.CompilerParams(vmem_limit_bytes=16 << 20),
        name="joined_columns",
    )(jnp.asarray(turned, jnp.int32).reshape(1), pre, bias)


def down_split_kernel(half, rows_ref, out_ref):
    members, _, own = out_ref.shape
    unit = own // half
    for k in range(half):
        for member in range(members):
            at = (k * members + member) * unit
            out_ref[member, :, k * unit : (k + 1) * unit] = rows_ref[:, at : at + unit]


def down_split_units(rows, half):
    count, width = rows.shape
    return pl.pallas_call(
        functools.partial(down_split_kernel, half),
        out_shape=jax.ShapeDtypeStruct((block_size, count, width // block_size), rows.dtype),
        in_specs=[in_vmem],
        out_specs=in_vmem,
        compiler_params=pltpu.CompilerParams(vmem_limit_bytes=12 << 20),
        name="down_split",
    )(rows)


def down_join_kernel(half, parts_ref, out_ref):
    members, _, own = parts_ref.shape
    unit = own // half
    for k in range(half):
        for member in range(members):
            at = (k * members + member) * unit
            part = parts_ref[member, :, k * unit : (k + 1) * unit]
            out_ref[:, at : at + unit] = part.astype(wide)


def down_join_units(parts, half):
    members, count, own = parts.shape
    return pl.pallas_call(
        functools.partial(down_join_kernel, half),
        out_shape=jax.ShapeDtypeStruct((count, members * own), wide),
        in_specs=[in_vmem],
        out_specs=in_vmem,
        compiler_params=pltpu.CompilerParams(vmem_limit_bytes=12 << 20),
        name="down_join",
    )(parts)


def split_kernel(half, turned_ref, grads_ref, out_ref):
    members, _, both = out_ref.shape
    unit = both // (2 * half)
    for k in range(half):
        for member in range(members):
            at = (k * members + member) * unit
            parts = [grads_ref[j, :, at : at + unit] for j in range(2)]
            for j in range(2):
                value = jnp.where(turned_ref[0] == 1, parts[1 - j], parts[j])
                out_ref[member, :, (j * half + k) * unit : (j * half + k + 1) * unit] = value


def split_columns(grads, turned, half):
    _, rows, width = grads.shape
    return pl.pallas_call(
        functools.partial(split_kernel, half),
        out_shape=jax.ShapeDtypeStruct((block_size, rows, 2 * width // block_size), grads.dtype),
        in_specs=[in_smem, in_vmem],
        out_specs=in_vmem,
        compiler_params=pltpu.CompilerParams(vmem_limit_bytes=16 << 20),
        name="split_columns",
    )(jnp.asarray(turned, jnp.int32).reshape(1), grads)


def normed(values, scales):
    return values * lax.rsqrt(jnp.mean(values * values, -1, keepdims=True) + epsilon) * scales


def gated_unit(gate, up):
    return jax.nn.gelu(gate, approximate=True) * up


def times_rows(operand, weight):
    return lax.dot_general(
        operand, weight, (((1,), (1,)), ((), ())), preferred_element_type=wide
    )


def times(operand, weight):
    return jnp.dot(operand, weight, preferred_element_type=wide)


def row_sums(gradient, operand):
    return lax.dot_general(
        gradient, operand, (((0,), (0,)), ((), ())), preferred_element_type=wide
    )


def gain_sums(gradient, weight):
    return jnp.sum(gradient * weight.astype(wide), 0)


def member_columns(values):
    rows, width = values.shape
    count = lax.axis_size("g")
    split = values.reshape(rows, count, block_size, width // (count * block_size))
    return split.transpose(2, 0, 1, 3).reshape(block_size, rows, width // block_size)


def after(values, earlier):
    return lax.optimization_barrier((values, earlier))[0]


class Exchange:
    def __init__(self, values):
        self.values = values
        self.share = 0
        self.parts = []

    def next(self, share):
        tiles = self.values.shape[0] // 16
        start = tiles * self.share // 16 * 16
        self.share += share
        return self.values, start, tiles * self.share // 16 * 16 - start

    def shift(self, share, earlier):
        values, start, size = self.next(share)
        part = lax.slice_in_dim(values, start, start + size, axis=0)
        part = after(part, earlier)
        self.parts.append(group_shift(part, 1))

    def whole(self):
        return self.parts[0] if len(self.parts) == 1 else jnp.concatenate(self.parts, 0)


def sharing(paired, plan):
    if not paired:
        return ()
    return tuple(exchange.next(share) for exchange, share in plan)


def arrived(paired, plan, parts):
    if paired:
        for (exchange, _), part in zip(plan, parts):
            exchange.parts.append(part)


def body(
    inputs,
    gain_first,
    branch_weight,
    branch_bias,
    conv_weight,
    conv_bias,
    gate_weight,
    gate_bias,
    decay,
    out_weight,
    out_bias,
    gain_second,
    mlp_weight,
    down_weight,
    cotangent,
):
    source = inputs[0].astype(wide)
    rows, width = source.shape
    heads, head_width = gate_weight.shape[1:3]
    count = lax.axis_size("g")
    half = count // 2
    paired = count == 2
    turned = (lax.axis_index("g") == 1) if paired else False
    all_rows = block_size * rows
    position = (
        lax.axis_index("g") * 4 + lax.axis_index("b3") * 2 + lax.axis_index("b2")
    ).reshape(1)
    flat = (rows, width)
    small = (8, width)

    def in_turn(first, second):
        if not paired:
            return first, second
        return jnp.where(turned, second, first), jnp.where(turned, first, second)

    def turn_halves(values):
        if not paired:
            return values
        return jnp.where(turned, jnp.roll(values, width // 2, 1), values)

    def move(gathered, swapped, collective, plan):
        outs = block_move(gathered, swapped, collective, sharing(paired, plan))
        own = (gathered is not None) + len(swapped)
        arrived(paired, plan, outs[own:])
        return outs[0] if own == 1 else outs[:own]

    def scatter(products, collective, plan, extra=None):
        out, *parts = block_scatter(products, collective, sharing(paired, plan), extra)
        arrived(paired, plan, parts)
        return out

    def joined(values, exchange):
        if paired:
            return jnp.concatenate([values, exchange.whole()], 0)
        return group_gather(values).reshape(-1, values.shape[1])

    def total(own, exchange, sums):
        if paired:
            return own + exchange.whole().astype(wide)
        return group_sum(sums)

    down_rows, hidden_width = down_weight.shape
    unit = hidden_width // (half * block_size)
    down_split = down_split_units(down_weight, half)
    mlp_trade = Exchange(mlp_weight)
    branch_trade = Exchange(branch_weight)
    out_rows = lax.all_gather(out_weight, places, axis=0, tiled=True)

    first_in = normed(source, gain_first).astype(low)
    first_all, down_own = move(
        first_in, (down_split,), 1, [(branch_trade, 16), (mlp_trade, 2)]
    )
    down_own = down_own.reshape(block_size * down_rows, half * unit)
    down_trade = Exchange(down_own)
    first_all = first_all.reshape(all_rows, width)
    cot_in = after(turn_halves(cotangent[0]), first_all)
    cot_all = lax.all_gather(cot_in, cube, axis=0, tiled=True)
    grad_out = cotangent[0]
    branch_rows = joined(branch_weight, branch_trade)
    pre_part = times_rows(first_all, branch_rows).astype(low)
    pre_part = pre_part.reshape(block_size, rows, 2 * width // block_size)
    pre = move(None, (pre_part,), 2, [(mlp_trade, 7)])
    if paired:
        mlp_trade.shift(3, pre)
    gate_pre, conv_in = joined_columns(pre, branch_bias.reshape(2, width), turned, half)
    conv_before = rim_rows(conv_in[rows - 8 :], 1)

    rate = (-8.0 * jax.nn.softplus(decay))[None]
    decays, local, product, ends = by_heads(
        local_states_kernel,
        heads,
        head_width,
        (
            position,
            conv_in,
            conv_before,
            conv_weight,
            conv_bias[None],
            gate_weight,
            gate_bias,
            rate,
        ),
        [(flat, wide)] * 3 + [((2, width), wide)],
    )
    all_ends = seq_spread(ends, 3)
    if paired:
        mlp_trade.shift(4, all_ends)
    states, mixed, entry = by_heads(
        full_states_kernel,
        heads,
        head_width,
        (position, local, product, all_ends, gate_pre),
        [(flat, wide), (flat, low), (small, wide)],
    )
    middle = source + times_rows(mixed, out_rows) + out_bias

    second_in = normed(middle, gain_second).astype(low)
    second_all = move(second_in, (), 4, [(down_trade, 12)])
    if paired:
        down_trade.shift(4, second_all)
    second_all = second_all.reshape(all_rows, width)
    if paired:
        rows_a, rows_b = mlp_weight, mlp_trade.whole()
    else:
        mlp_rows = group_gather(mlp_weight)
        rows_a = mlp_rows[:half].reshape(-1, width)
        rows_b = mlp_rows[half:].reshape(-1, width)
    down_columns = joined(down_own, down_trade)
    pre_a = times_rows(second_all, rows_a)
    mlp_gate, mlp_up = in_turn(pre_a, times_rows(second_all, rows_b))
    mlp_hidden, gated_back = jax.vjp(gated_unit, mlp_gate, mlp_up)
    mlp_hidden = mlp_hidden.astype(low)
    grad_hidden = times(cot_all, down_columns)
    grad_a, grad_b = in_turn(*(grad.astype(low) for grad in gated_back(grad_hidden)))
    sum_b = row_sums(grad_b, second_all)
    sum_b_low = sum_b.astype(low)
    mlp_back = Exchange(sum_b_low)
    grad_second = scatter(
        [(grad_a, rows_a, False), (grad_b, rows_b, False)], 5, [(mlp_back, 8)]
    )
    down_sum = row_sums(cot_all, mlp_hidden)
    down_sums = down_sum.astype(low).reshape(count, block_size * down_rows, half * unit)
    down_back = Exchange(down_sums[1])
    down_left = after(mlp_hidden, grad_second)
    down_full = scatter([(down_left, down_columns, True)], 6, [(mlp_back, 8)])
    output = (middle + turn_halves(down_full)).astype(low)[None]
    if paired:
        down_back.shift(5, down_full)

    _, second_back = jax.vjp(normed, middle, gain_second)
    grad_mid_norm, gain_second_term = second_back(grad_second)
    grad_middle = grad_out.astype(wide) + grad_mid_norm
    grad_branch = grad_middle.astype(low)
    out_bias_term = jnp.sum(grad_branch.astype(wide), 0)
    grad_mixed = times(grad_branch, out_rows)

    adjoint, tail, adjoint_ends = by_heads(
        local_adjoint_kernel,
        heads,
        head_width,
        (grad_mixed, gate_pre, decays),
        [(flat, wide), (flat, wide), ((2, width), wide)],
    )
    all_adjoint_ends = seq_spread(adjoint_ends, 9)
    mixed_all = lax.all_gather(after(mixed, down_full), cube, axis=0, tiled=True)
    if paired:
        down_back.shift(9, all_adjoint_ends)
    grad_conv, gate_weight_term, gate_sums = by_heads(
        gate_grads_kernel,
        heads,
        head_width,
        (
            position,
            adjoint,
            tail,
            all_adjoint_ends,
            decays,
            states,
            entry,
            conv_in,
            conv_before,
            conv_weight,
            conv_bias[None],
            gate_weight,
            gate_bias,
            rate,
        ),
        [(flat, wide), ((2, head_width, width), low), (small, wide)],
    )
    conv_after = rim_rows(grad_conv[:8], -1)
    pre_grads, pre_sums = by_heads(
        branch_grads_kernel,
        heads,
        head_width,
        (grad_conv, conv_after, conv_weight, gate_pre, grad_mixed, states),
        [((2, rows, width), low), (small, wide)],
    )

    columns = split_columns(pre_grads, turned, half)
    pre_all, branch_all = move(None, (columns, member_columns(grad_branch)), 10, [])
    branch_all = branch_all.reshape(all_rows, -1)
    out_sum = row_sums(branch_all, mixed_all).reshape(count, -1, width)
    out_sums = out_sum.astype(low)
    own_out, other_out = in_turn(out_sum[0], out_sum[1])
    out_back = Exchange(other_out.astype(low))
    if paired:
        down_back.shift(2, pre_all)
    pre_all = pre_all.reshape(all_rows, -1)
    branch_sum = row_sums(pre_all, first_all)
    branch_sums = branch_sum.astype(low).reshape(count, -1, width)
    branch_back = Exchange(branch_sums[1])
    gain_first_term = gain_sums(branch_sum, branch_rows)

    tops = jnp.stack([out_bias_term, gain_first_term, gain_second_term], 0)
    vectors = jnp.concatenate([gate_sums, pre_sums[:2], tops, jnp.zeros((3, width), wide)], 0)
    vectors = vectors.astype(low)
    gate_terms = gate_weight_term.reshape(block_size, -1, width)
    gate_unit = gate_terms.shape[1]
    shared_part = jnp.concatenate(
        [
            gate_terms,
            vectors[:, None, :],
            jnp.zeros((block_size, 15, width), low),
        ],
        1,
    )
    scattered = scatter(
        [(pre_all, branch_rows, False)], 11, [(branch_back, 10), (out_back, 16)], shared_part
    )
    grad_first = scattered[:rows]
    _, first_back = jax.vjp(lambda values: normed(values, gain_first), source)
    input_grad = (grad_middle + first_back(grad_first)[0])[None]
    shared = group_total(scattered[rows:]).astype(low)
    sum_a = row_sums(after(grad_a, scattered), second_all)
    mlp_low = jnp.concatenate([sum_a.astype(low), sum_b_low], 0).reshape(count, -1, width)
    mlp_grad = total(sum_a, mlp_back, mlp_low)

    if paired:
        down_total = down_sum[: block_size * down_rows] + down_back.whole().astype(wide)
    else:
        down_total = group_sum(down_sums)
    down_total = down_total.astype(low).reshape(block_size, down_rows, half * unit)
    shared_all, down_total = move(shared, (down_total,), 7, [(branch_back, 6)])
    down_grad = down_join_units(down_total, half)
    gate_sum = shared_all[:, :gate_unit].reshape(2, head_width, width)
    gate_weight_grad = jnp.stack(
        [gate_sum[:, :, h * head_width : (h + 1) * head_width] for h in range(heads)], 1
    ).astype(wide)
    sums = shared_all[:, gate_unit].astype(wide)
    branch_grad = total(branch_sum[: branch_weight.shape[0]], branch_back, branch_sums)
    out_grad = total(own_out, out_back, out_sums)
    return (
        output,
        input_grad,
        sums[11] / gain_first,
        branch_grad,
        sums[8:10].reshape(-1),
        sums[4:8],
        sums[3],
        gate_weight_grad,
        sums[:2],
        sums[2] * (-8.0 * jax.nn.sigmoid(decay)),
        out_grad,
        sums[10],
        sums[12],
        mlp_grad,
        down_grad,
    )


def solution(mesh):
    count = mesh.devices.size // block_size
    blocks = Mesh(mesh.devices.reshape((count,) + (2,) * len(cube)), places)
    tokens = P(fsdp_axes, seq_axes, None)
    owned = P(places, None)
    return jax.shard_map(
        body,
        mesh=blocks,
        in_specs=(
            tokens,
            P(),
            owned,
            P(),
            P(),
            P(),
            P(),
            P(),
            P(),
            owned,
            P(),
            P(),
            owned,
            owned,
            tokens,
        ),
        out_specs=(
            tokens,
            tokens,
            P(),
            owned,
            P(),
            P(),
            P(),
            P(),
            P(),
            P(),
            owned,
            P(),
            P(),
            owned,
            owned,
        ),
        check_vma=False,
    )
```

```python
import functools

import jax
import jax.numpy as jnp
from jax import lax
from jax.experimental import pallas as pl
from jax.experimental.pallas import tpu as pltpu
from jax.sharding import Mesh
from jax.sharding import PartitionSpec as P

epsilon = 1e-06
low = jnp.bfloat16
wide = jnp.float32

cube = ("b3", "b2", "b1", "b0")
block_size = 16
places = ("g",) + cube
seq_axes = ("g", "b3", "b2")
fsdp_axes = ("b1", "b0")
first_orders = (("b3", "b1", "b2"), ("b3", "b2", "b1"))
even_orders = (("b1", "b3", "b2"), ("b2", "b3", "b1"))

anywhere = pl.BlockSpec(memory_space=pl.ANY)
in_vmem = pl.BlockSpec(memory_space=pltpu.VMEM)
in_smem = pl.BlockSpec(memory_space=pltpu.SMEM)
whole_vmem = 67000000


def bit_of(axis):
    return 1 << (len(cube) - 1 - cube.index(axis))


def slot_at(mask):
    slot = 0
    for axis in cube:
        here = lax.axis_index(axis)
        slot = slot * 2 + (1 - here if mask & bit_of(axis) else here)
    return slot


def device_at(mask):
    return {axis: 1 - lax.axis_index(axis) for axis in cube if mask & bit_of(axis)}


def greet(masks, paired):
    barrier = pltpu.get_barrier_semaphore()
    targets = [device_at(mask) for mask in masks] + [other_block()] * paired
    for target in targets:
        pl.semaphore_signal(
            barrier, inc=1, device_id=target, device_id_type=pl.DeviceIdType.MESH
        )
    pl.semaphore_wait(barrier, len(targets))


def other_block():
    return {"g": 1 - lax.axis_index("g")}


class Ride:
    def __init__(self, riders):
        self.arrays = [array for array, _, _ in riders]
        self.ranges = [(start, size) for _, start, size in riders]
        self.chunks = []
        for number, (array, start, size) in enumerate(riders):
            step = 16 if array.shape[1] > 4096 else (48 if array.shape[1] > 1024 else 160)
            for begin in range(0, size, step):
                self.chunks.append((number, start + begin, begin, min(step, size - begin)))

    def shapes(self):
        return [
            jax.ShapeDtypeStruct((size,) + array.shape[1:], array.dtype)
            for array, (_, size) in zip(self.arrays, self.ranges)
        ]

    def semaphores(self):
        count = max(1, len(self.chunks))
        return [pltpu.SemaphoreType.DMA((count,)), pltpu.SemaphoreType.DMA((count,))]

    def enter(self, inputs, outputs, send_sem, recv_sem):
        self.copies = [
            pltpu.make_async_remote_copy(
                src_ref=inputs[number].at[pl.ds(begin, size)],
                dst_ref=outputs[number].at[pl.ds(start, size)],
                send_sem=send_sem.at[chunk],
                recv_sem=recv_sem.at[chunk],
                device_id=other_block(),
                device_id_type=pl.DeviceIdType.MESH,
            )
            for chunk, (number, begin, start, size) in enumerate(self.chunks)
        ]
        self.started = 0

    def start(self, share):
        until = -(-len(self.copies) * share[0] // share[1])
        for copy in self.copies[self.started : until]:
            copy.start()
        self.started = max(self.started, until)

    def finish(self):
        self.start((1, 1))
        for copy in self.copies:
            copy.wait()


def split_rows(rows, orders):
    tiles = rows // 16
    pieces = []
    start = 0
    for number, order in enumerate(orders):
        size = (tiles + len(orders) - 1 - number) // len(orders) * 16
        if size:
            pieces.append((order, start, size))
        start += size
    return pieces


def hop_orders(riders):
    return first_orders + even_orders if riders else even_orders


def remote_params(collective, held):
    return pltpu.CompilerParams(
        collective_id=collective,
        has_side_effects=True,
        vmem_limit_bytes=min(whole_vmem, held + (2 << 20)),
    )


def bytes_of(*values):
    return sum(value.size * value.dtype.itemsize for value in values)


def move_kernel(pieces, swap_count, ride, *refs):
    refs = list(refs)

    def take(count):
        taken = refs[:count]
        del refs[:count]
        return taken

    gathers = 1 if pieces else 0
    count = len(ride.arrays)
    sources, swaps, riders = take(gathers), take(swap_count), take(count)
    targets, swapped, arrivals = take(gathers), take(swap_count), take(count)
    send_sem, recv_sem, local_sem, swap_send, swap_recv, ride_send, ride_recv = refs
    neighbours = [bit_of(axis) for axis in cube]
    greet(list(range(1, block_size)) if swap_count else neighbours, count > 0)
    ride.enter(riders, arrivals, ride_send, ride_recv)
    sent = []
    here = slot_at(0)
    locals_ = []

    def push(part, start, size, mask, axis):
        slot = slot_at(mask)
        source = (sources[0] if mask == 0 else targets[0].at[slot]).at[pl.ds(start, size)]
        copy = pltpu.make_async_remote_copy(
            src_ref=source,
            dst_ref=targets[0].at[slot].at[pl.ds(start, size)],
            send_sem=send_sem.at[len(sent)],
            recv_sem=recv_sem.at[part, mask ^ bit_of(axis)],
            device_id=device_at(bit_of(axis)),
            device_id_type=pl.DeviceIdType.MESH,
        )
        copy.start()
        sent.append(copy)

    def arrive(part, start, size, mask):
        target = targets[0].at[slot_at(mask)].at[pl.ds(start, size)]
        pltpu.make_async_copy(target, target, recv_sem.at[part, mask]).wait()

    def forward(stage):
        for part, (order, start, size) in enumerate(pieces):
            order = order + ("b0",)
            masks = [0]
            if stage > 0:
                for axis in order[: stage - 1]:
                    masks = masks + [mask | bit_of(axis) for mask in masks]
                masks = [mask | bit_of(order[stage - 1]) for mask in masks]
            for mask in masks:
                if mask:
                    arrive(part, start, size, mask)
                for axis in order[stage:]:
                    push(part, start, size, mask, axis)

    forward(0)
    swap_copies = []
    for mask in (15, 14, 13, 11, 7, 12, 10, 6, 9, 5, 3, 8, 4, 2, 1):
        for number in range(swap_count):
            copy = pltpu.make_async_remote_copy(
                src_ref=swaps[number].at[slot_at(mask)],
                dst_ref=swapped[number].at[here],
                send_sem=swap_send.at[number, mask],
                recv_sem=swap_recv.at[number, mask],
                device_id=device_at(mask),
                device_id_type=pl.DeviceIdType.MESH,
            )
            copy.start()
            swap_copies.append(copy)
    ride.start((1, 1))
    for number in range(gathers):
        locals_.append((sources[number], targets[number].at[here]))
    for number in range(swap_count):
        locals_.append((swaps[number].at[here], swapped[number].at[here]))
    locals_ = [
        pltpu.make_async_copy(source, target, local_sem.at[number])
        for number, (source, target) in enumerate(locals_)
    ]
    for copy in locals_:
        copy.start()
    for stage in (1, 2, 3):
        forward(stage)
    for part, (_, start, size) in enumerate(pieces):
        for mask in range(block_size):
            if mask & bit_of("b0"):
                arrive(part, start, size, mask)
    for number in range(swap_count):
        for mask in range(1, block_size):
            target = swapped[number].at[slot_at(mask)]
            pltpu.make_async_copy(target, target, swap_recv.at[number, mask]).wait()
    for copy in sent + swap_copies:
        copy.wait_send()
    for copy in locals_:
        copy.wait()
    ride.finish()


def block_move(gathered, swapped, collective, riders=()):
    pieces = []
    shapes = []
    gathers = [] if gathered is None else [gathered]
    for values in gathers:
        pieces = split_rows(values.shape[0], hop_orders(riders))
        shapes.append(jax.ShapeDtypeStruct((block_size,) + values.shape, values.dtype))
    for values in swapped:
        shapes.append(jax.ShapeDtypeStruct(values.shape, values.dtype))
    ride = Ride(riders)
    swaps = max(1, len(swapped))
    moved = len(gathers) * [anywhere] + len(swapped) * [in_vmem] + len(riders) * [anywhere]
    return pl.pallas_call(
        functools.partial(move_kernel, pieces, len(swapped), ride),
        out_shape=shapes + ride.shapes(),
        in_specs=len(gathers) * [in_vmem] + moved[len(gathers) :],
        out_specs=moved,
        scratch_shapes=[
            pltpu.SemaphoreType.DMA((max(1, 15 * len(pieces)),)),
            pltpu.SemaphoreType.DMA((max(1, len(pieces)), block_size)),
            pltpu.SemaphoreType.DMA((1 + swaps,)),
            pltpu.SemaphoreType.DMA((swaps, block_size)),
            pltpu.SemaphoreType.DMA((swaps, block_size)),
        ]
        + ride.semaphores(),
        compiler_params=remote_params(
            collective, 2 * bytes_of(*gathers) + 4 * bytes_of(*swapped)
        ),
        name="block_move",
    )(*gathers, *swapped, *ride.arrays)


def scatter_kernel(pieces, product_rows, transposed, extra_count, ride, *refs):
    refs = list(refs)

    def take(count):
        taken = refs[:count]
        del refs[:count]
        return taken

    products = len(transposed)
    count = len(ride.arrays)
    left_refs, right_refs, extras, riders = (
        take(products),
        take(products),
        take(extra_count),
        take(count),
    )
    (out_ref,), arrivals = take(1), take(count)
    left_rows = take(products)
    held, away, send_sem, recv_sem, left_sem, load_sem, ride_send, ride_recv = refs
    core = bit_of("b0")
    members = 2 * product_rows
    order_count = [sum(mask >> bit & 1 for bit in range(len(cube))) for mask in range(block_size)]
    steps = sorted(
        (mask for mask in range(block_size) if not mask & core),
        key=lambda mask: (-order_count[mask], -mask),
    )
    here = lax.axis_index("b0")

    def left_copy(number, step):
        pair = slot_at(steps[step]) // 2
        rows = pl.ds(pl.multiple_of(pair * members, members), members)
        return pltpu.make_async_copy(
            left_refs[number].at[rows], left_rows[number].at[step], left_sem.at[number, step]
        )

    for step in range(8):
        for number in range(products):
            left_copy(number, step).start()
    greet([bit_of(axis) for axis in cube], count > 0)
    ride.enter(riders, arrivals, ride_send, ride_recv)
    sent = []

    def slot_of(order, hop, mask):
        clear = [bit_of(axis) for axis in order[:hop]] + [core]
        masks = [m for m in range(block_size) if not any(m & bit for bit in clear)]
        return (0, 8, 12, 14)[hop] + masks.index(mask)

    def push(source, number, slot, axis):
        _, _, _, start, size = pieces[number]
        copy = pltpu.make_async_remote_copy(
            src_ref=source,
            dst_ref=away.at[slot].at[pl.ds(start, size)],
            send_sem=send_sem.at[len(sent)],
            recv_sem=recv_sem.at[number, slot],
            device_id=device_at(bit_of(axis)),
            device_id_type=pl.DeviceIdType.MESH,
        )
        copy.start()
        sent.append(copy)

    def arrive(number, slot):
        _, _, _, start, size = pieces[number]
        target = away.at[slot].at[pl.ds(start, size)]
        pltpu.make_async_copy(target, target, recv_sem.at[number, slot]).wait()

    tile = 512

    def work_out(step):
        for number in range(products):
            left_copy(number, step).wait()

        def columns(i, carry):
            at = pl.ds(pl.multiple_of(i * tile, tile), tile)
            total = None
            for number in range(products):
                left = left_rows[number][step]
                if transposed[number]:
                    term = lax.dot_general(
                        left,
                        right_refs[number][at, :],
                        (((1,), (1,)), ((), ())),
                        preferred_element_type=wide,
                    )
                else:
                    term = jnp.dot(left, right_refs[number][:, at], preferred_element_type=wide)
                total = term if total is None else total + term
            total = total.astype(low)
            held[step, 0, pl.ds(0, product_rows), at] = total[:product_rows]
            held[step, 1, pl.ds(0, product_rows), at] = total[product_rows:]
            return carry

        lax.fori_loop(0, out_ref.shape[1] // tile, columns, 0)
        for number, (order, extra, begin, start, size) in enumerate(pieces):
            rows = pl.ds(begin, size)
            if extra:
                source = extras[0].at[slot_at(steps[step] | core)].at[rows]
            else:
                source = held.at[step, 1 - here].at[rows]
            push(source, number, slot_of(order, 0, steps[step]), "b0")

    loads = {}
    for step in range(8):
        for number, (order, extra, begin, start, size) in enumerate(pieces):
            if extra:
                loads[number, step] = pltpu.make_async_copy(
                    extras[0].at[slot_at(steps[step])].at[pl.ds(begin, size)],
                    held.at[step, here].at[pl.ds(start, size)],
                    load_sem.at[number, step],
                )
                loads[number, step].start()

    def pass_on(step):
        mask = steps[step]
        for number, (order, extra, begin, start, size) in enumerate(pieces):
            bits = [bit_of(axis) for axis in order]
            if extra:
                loads[number, step].wait()
            slots = [slot_of(order, 0, mask)]
            target = None
            for hop, bit in enumerate(bits):
                if mask & bit:
                    target = hop
                    break
                slots.append(slot_of(order, hop + 1, mask))
            for slot in slots:
                arrive(number, slot)

            def add_tile(i, carry, start=start, slots=slots, target=target):
                at = pl.ds(pl.multiple_of(start + i * 16, 16), 16)
                total = held[step, here, at, :].astype(wide)
                for slot in slots:
                    total = total + away[slot, at, :].astype(wide)
                if target is None:
                    out_ref[at, :] = total.astype(out_ref.dtype)
                else:
                    held[step, here, at, :] = total.astype(low)
                return carry

            lax.fori_loop(0, size // 16, add_tile, 0)
            if target is not None:
                push(
                    held.at[step, here].at[pl.ds(start, size)],
                    number,
                    slot_of(order, target + 1, mask ^ bits[target]),
                    order[target],
                )

    for step in range(9):
        if step < 8:
            work_out(step)
        if step == 0:
            ride.start((1, 1))
        if step > 0:
            pass_on(step - 1)
    for copy in sent:
        copy.wait_send()
    ride.finish()


def block_scatter(products, collective, riders=(), extra=None):
    ride = Ride(riders)
    lefts = [left for left, _, _ in products]
    rights = [right for _, right, _ in products]
    transposed = [flag for _, _, flag in products]
    product_rows = lefts[0].shape[0] // block_size
    width = rights[0].shape[0] if transposed[0] else rights[0].shape[1]
    extras = [] if extra is None else [extra]
    orders = [order[::-1] for order in hop_orders(riders)]
    pieces = [
        (order, 0, start, start, size) for order, start, size in split_rows(product_rows, orders)
    ]
    rows = product_rows
    for values in extras:
        for order, start, size in split_rows(values.shape[1], orders):
            pieces.append((order, 1, start, rows + start, size))
        rows += values.shape[1]
    padded = [-(-left.shape[1] // 128) * 128 for left in lefts]
    held_bytes = (
        (16 + 15) * rows * width * 2
        + 2 * rows * width * 4
        + sum(2 * left.shape[0] * size for left, size in zip(lefts, padded))
        + 2 * sum(2 * size * width for size in padded)
        + (8 << 20)
    )
    return pl.pallas_call(
        functools.partial(
            scatter_kernel, pieces, product_rows, transposed, len(extras), ride
        ),
        out_shape=[jax.ShapeDtypeStruct((rows, width), wide)] + ride.shapes(),
        in_specs=[anywhere] * len(lefts)
        + [in_vmem] * len(rights)
        + [anywhere] * (len(extras) + len(riders)),
        out_specs=[in_vmem] + [anywhere] * len(riders),
        scratch_shapes=[pltpu.VMEM((8, 2 * product_rows, left.shape[1]), low) for left in lefts]
        + [
            pltpu.VMEM((8, 2, rows, width), low),
            pltpu.VMEM((15, rows, width), low),
            pltpu.SemaphoreType.DMA((15 * len(pieces),)),
            pltpu.SemaphoreType.DMA((len(pieces), 15)),
            pltpu.SemaphoreType.DMA((len(lefts), 8)),
            pltpu.SemaphoreType.DMA((len(pieces), 8)),
        ]
        + ride.semaphores(),
        compiler_params=remote_params(collective, held_bytes),
        name="block_scatter",
    )(*lefts, *rights, *extras, *ride.arrays)


def group_shift(values, distance):
    count = lax.axis_size("g")
    return lax.ppermute(values, "g", [(i, (i + distance) % count) for i in range(count)])


def group_gather(values):
    return lax.all_gather(values, "g", axis=0)


def group_sum(partials):
    return lax.psum_scatter(partials.astype(low), "g", scatter_dimension=0).astype(wide)


def group_total(values):
    count = lax.axis_size("g")
    total = values
    for distance in range(1, count):
        total = total + group_shift(values.astype(low), distance).astype(wide)
    return total


def spread_kernel(group_count, x_ref, out_ref, send_sem, recv_sem, local_sem):
    here_g, here_3, here_2 = (lax.axis_index(axis) for axis in seq_axes)
    peers = []
    for step in range(group_count):
        for mask in range(4):
            if step or mask:
                peers.append((step, mask))

    def place(step, mask):
        return (
            lax.rem(here_g + step, group_count),
            1 - here_3 if mask & 2 else here_3,
            1 - here_2 if mask & 1 else here_2,
        )

    barrier = pltpu.get_barrier_semaphore()
    for step, mask in peers:
        pl.semaphore_signal(
            barrier,
            inc=1,
            device_id=dict(zip(seq_axes, place(step, mask))),
            device_id_type=pl.DeviceIdType.MESH,
        )
    pl.semaphore_wait(barrier, len(peers))
    mine = here_g * 4 + here_3 * 2 + here_2
    sent = []
    for number, (step, mask) in enumerate(peers):
        copy = pltpu.make_async_remote_copy(
            src_ref=x_ref,
            dst_ref=out_ref.at[mine],
            send_sem=send_sem.at[number],
            recv_sem=recv_sem.at[number],
            device_id=dict(zip(seq_axes, place(step, mask))),
            device_id_type=pl.DeviceIdType.MESH,
        )
        copy.start()
        sent.append(copy)
    own = pltpu.make_async_copy(x_ref, out_ref.at[mine], local_sem)
    own.start()
    for number, (step, mask) in enumerate(peers):
        from_g, from_3, from_2 = place(group_count - step, mask)
        target = out_ref.at[from_g * 4 + from_3 * 2 + from_2]
        pltpu.make_async_copy(target, target, recv_sem.at[number]).wait()
    for copy in sent:
        copy.wait_send()
    own.wait()


def seq_spread(values, collective):
    group_count = lax.axis_size("g")
    count = 4 * group_count
    return pl.pallas_call(
        functools.partial(spread_kernel, group_count),
        out_shape=jax.ShapeDtypeStruct((count,) + values.shape, values.dtype),
        in_specs=[in_vmem],
        out_specs=in_vmem,
        scratch_shapes=[
            pltpu.SemaphoreType.DMA((count,)),
            pltpu.SemaphoreType.DMA((count,)),
            pltpu.SemaphoreType.DMA,
        ],
        compiler_params=remote_params(collective, 2 * (count + 1) * 8 * bytes_of(values)),
        name="seq_spread",
    )(values)


def rim_rows(values, offset):
    count = 4 * lax.axis_size("g")
    route = [(i - offset, i) for i in range(count) if 0 <= i - offset < count]
    return lax.ppermute(values, seq_axes, route)


def gelu_parts(v):
    inner = 0.7978845608028654 * (v + 0.044715 * v * v * v)
    t = jnp.tanh(inner)
    value = 0.5 * v * (1.0 + t)
    slope = 0.5 * (1.0 + t) + 0.5 * v * (1.0 - t * t) * 0.7978845608028654 * (
        1.0 + 0.134145 * v * v
    )
    return value, slope


def shifted(values, distance, fill):
    rows = values.shape[0]
    if distance % 8 == 0:
        head = jnp.full((distance,) + values.shape[1:], fill, values.dtype)
        return jnp.concatenate([head, values[: rows - distance]], 0)
    row = lax.broadcasted_iota(jnp.int32, values.shape, 0)
    return jnp.where(row >= distance, pltpu.roll(values, distance, 0), fill)


def shifted_back(values, distance, fill):
    rows = values.shape[0]
    if distance % 8 == 0:
        tail = jnp.full((distance,) + values.shape[1:], fill, values.dtype)
        return jnp.concatenate([values[distance:], tail], 0)
    row = lax.broadcasted_iota(jnp.int32, values.shape, 0)
    return jnp.where(row < rows - distance, pltpu.roll(values, rows - distance, 0), fill)


def scan_rows(rates, terms, shift):
    distance = 1
    while distance < rates.shape[0]:
        terms = terms + rates * shift(terms, distance, 0.0)
        rates = rates * shift(rates, distance, 1.0)
        distance *= 2
    return rates, terms


def one_minus_square(log_rate):
    x = 2.0 * log_rate
    series = 1.0
    for n in (9, 8, 7, 6, 5, 4, 3, 2):
        series = 1.0 + x * (1.0 / n) * series
    return jnp.where(x > -0.5, -x * series, 1.0 - jnp.exp(x))


def lagged_sum(ext, weights, start):
    total = start
    for lag in range(weights.shape[0]):
        moved = pltpu.roll(ext, lag, 0) if lag else ext
        total = total + weights[lag : lag + 1, :] * moved[8:, :]
    return total


def opening_rows(shape, position):
    return (lax.broadcasted_iota(jnp.int32, shape, 0) == 0) & (position == 0)


def conv_and_gates(conv_in_ref, before_ref, taps_ref, bias_ref, weight_ref, gate_bias_ref):
    ext = jnp.concatenate([before_ref[...], conv_in_ref[...]], 0)
    conv_out = lagged_sum(ext, taps_ref[...], bias_ref[...])
    conv_low = conv_out.astype(low)
    gates = [
        jax.nn.sigmoid(
            jnp.dot(conv_low, weight_ref[j, 0], preferred_element_type=wide)
            + gate_bias_ref[j : j + 1, :]
        )
        for j in range(2)
    ]
    return ext, conv_out, conv_low, gates


def local_states_kernel(
    position_ref,
    conv_in_ref,
    before_ref,
    taps_ref,
    bias_ref,
    weight_ref,
    gate_bias_ref,
    rate_ref,
    decay_ref,
    local_ref,
    product_ref,
    ends_ref,
):
    _, conv_out, _, gates = conv_and_gates(
        conv_in_ref, before_ref, taps_ref, bias_ref, weight_ref, gate_bias_ref
    )
    log_rate = rate_ref[...] * gates[0]
    rates = jnp.exp(log_rate)
    scaling = jnp.where(
        opening_rows(rates.shape, position_ref[0]), 1.0, jnp.sqrt(one_minus_square(log_rate))
    )
    product, states = scan_rows(rates, scaling * gates[1] * conv_out, shifted)
    decay_ref[...] = rates
    local_ref[...] = states
    product_ref[...] = product
    rows = rates.shape[0]
    ends_ref[...] = jnp.concatenate(
        [
            product[rows - 1 :],
            states[rows - 1 :],
        ],
        0,
    )


def full_states_kernel(
    position_ref, local_ref, product_ref, ends_ref, gate_pre_ref, states_ref, mixed_ref, entry_ref
):
    entry = jnp.zeros((1, local_ref.shape[1]), wide)
    for s in range(ends_ref.shape[0]):
        later = ends_ref[s, 0:1, :] * entry + ends_ref[s, 1:2, :]
        entry = jnp.where(s < position_ref[0], later, entry)
    states = local_ref[...] + product_ref[...] * entry
    states_ref[...] = states
    mixed_ref[...] = (states * gelu_parts(gate_pre_ref[...])[0]).astype(low)
    entry_ref[...] = jnp.broadcast_to(entry, entry_ref.shape)


def local_adjoint_kernel(
    grad_mixed_ref, gate_pre_ref, decay_ref, local_ref, product_ref, ends_ref
):
    grad_states = grad_mixed_ref[...] * gelu_parts(gate_pre_ref[...])[0]
    rates = decay_ref[...]
    product, adjoint = scan_rows(shifted_back(rates, 1, 1.0), grad_states, shifted_back)
    local_ref[...] = adjoint
    product_ref[...] = product
    ends_ref[...] = jnp.concatenate(
        [
            rates[0:1] * product[0:1],
            rates[0:1] * adjoint[0:1],
        ],
        0,
    )


def gate_grads_kernel(
    position_ref,
    local_ref,
    product_ref,
    ends_ref,
    decay_ref,
    states_ref,
    entry_ref,
    conv_in_ref,
    before_ref,
    taps_ref,
    bias_ref,
    weight_ref,
    gate_bias_ref,
    rate_ref,
    grad_conv_ref,
    weight_grad_ref,
    sums_ref,
):
    position = position_ref[0]
    entry = jnp.zeros((1, local_ref.shape[1]), wide)
    for s in range(ends_ref.shape[0] - 1, 0, -1):
        earlier = ends_ref[s, 0:1, :] * entry + ends_ref[s, 1:2, :]
        entry = jnp.where(s > position, earlier, entry)
    adjoint = local_ref[...] + product_ref[...] * entry
    rates = decay_ref[...]
    ext, conv_out, conv_low, (rgate, igate) = conv_and_gates(
        conv_in_ref, before_ref, taps_ref, bias_ref, weight_ref, gate_bias_ref
    )
    row = lax.broadcasted_iota(jnp.int32, rates.shape, 0)
    before = jnp.where(row == 0, entry_ref[0:1, :], pltpu.roll(states_ref[...], 1, 0))
    opening = opening_rows(rates.shape, position)
    log_rate = rate_ref[...] * rgate
    root = jnp.sqrt(one_minus_square(log_rate))
    scaling = jnp.where(opening, 1.0, root)
    grad_scaling = adjoint * igate * conv_out
    grad_log = adjoint * before * rates - jnp.where(
        opening, 0.0, grad_scaling * rates * rates / root
    )
    grad_rgate = grad_log * rate_ref[...] * rgate * (1.0 - rgate)
    grad_igate = adjoint * scaling * conv_out * igate * (1.0 - igate)
    grad_conv = adjoint * scaling * igate
    sums = []
    for j, grad in enumerate((grad_rgate, grad_igate)):
        grad_low = grad.astype(low)
        sums.append(jnp.sum(grad_low.astype(wide), 0, keepdims=True))
        weight_grad_ref[j] = lax.dot_general(
            conv_low, grad_low, (((0,), (0,)), ((), ())), preferred_element_type=wide
        ).astype(low)
        grad_conv = grad_conv + lax.dot_general(
            grad_low, weight_ref[j, 0], (((1,), (1,)), ((), ())), preferred_element_type=wide
        )
    grad_conv_ref[...] = grad_conv
    sums.append(jnp.sum(grad_log * rgate, 0, keepdims=True))
    sums.append(jnp.sum(grad_conv, 0, keepdims=True))
    for lag in range(4):
        moved = pltpu.roll(ext, lag, 0) if lag else ext
        sums.append(jnp.sum(grad_conv * moved[8:, :], 0, keepdims=True))
    sums_ref[...] = jnp.concatenate(sums, 0)


def branch_grads_kernel(
    grad_conv_ref, after_ref, taps_ref, gate_pre_ref, grad_mixed_ref, states_ref, out_ref, sums_ref
):
    grad_conv = grad_conv_ref[...]
    rows = grad_conv.shape[0]
    ext = jnp.concatenate([grad_conv, after_ref[...]], 0)
    total = taps_ref[0:1, :] * grad_conv
    for lag in range(1, taps_ref.shape[0]):
        moved = pltpu.roll(ext, rows + 8 - lag, 0)
        total = total + taps_ref[lag : lag + 1, :] * moved[:rows, :]
    slope = gelu_parts(gate_pre_ref[...])[1]
    grad_gate = slope * grad_mixed_ref[...] * states_ref[...]
    sums = []
    for j, grad in enumerate((grad_gate, total)):
        grad_low = grad.astype(low)
        out_ref[j] = grad_low
        sums.append(jnp.sum(grad_low.astype(wide), 0, keepdims=True))
    sums_ref[...] = jnp.concatenate(sums + [jnp.zeros((6, grad_conv.shape[1]), wide)], 0)


def by_heads(kernel, heads, width, operands, outs):
    def spec(shape):
        if len(shape) == 1:
            return in_smem
        if len(shape) == 4:
            return pl.BlockSpec((shape[0], 1, width, width), lambda h: (0, h, 0, 0))
        lead = shape[:-1]
        return pl.BlockSpec(lead + (width,), lambda h, rank=len(lead): (0,) * rank + (h,))

    return pl.pallas_call(
        kernel,
        grid=(heads,),
        out_shape=[jax.ShapeDtypeStruct(shape, dtype) for shape, dtype in outs],
        in_specs=[spec(value.shape) for value in operands],
        out_specs=[spec(shape) for shape, _ in outs],
        compiler_params=pltpu.CompilerParams(vmem_limit_bytes=12 << 20),
    )(*operands)


def joined_kernel(half, turned_ref, pre_ref, bias_ref, *out_refs):
    members, _, both = pre_ref.shape
    unit = both // (2 * half)
    bias = bias_ref[...]
    for k in range(half):
        for member in range(members):
            parts = [
                pre_ref[member, :, (j * half + k) * unit : (j * half + k + 1) * unit].astype(wide)
                for j in range(2)
            ]
            at = (k * members + member) * unit
            for j in range(2):
                value = jnp.where(turned_ref[0] == 1, parts[1 - j], parts[j])
                out_refs[j][:, at : at + unit] = value + bias[j : j + 1, at : at + unit]


def joined_columns(pre, bias, turned, half):
    shape = jax.ShapeDtypeStruct((pre.shape[1], bias.shape[1]), wide)
    return pl.pallas_call(
        functools.partial(joined_kernel, half),
        out_shape=[shape, shape],
        in_specs=[in_smem, in_vmem, in_vmem],
        out_specs=[in_vmem, in_vmem],
        compiler_params=pltpu.CompilerParams(vmem_limit_bytes=16 << 20),
        name="joined_columns",
    )(jnp.asarray(turned, jnp.int32).reshape(1), pre, bias)


def down_split_kernel(half, rows_ref, out_ref):
    members, _, own = out_ref.shape
    unit = own // half
    for k in range(half):
        for member in range(members):
            at = (k * members + member) * unit
            out_ref[member, :, k * unit : (k + 1) * unit] = rows_ref[:, at : at + unit]


def down_split_units(rows, half):
    count, width = rows.shape
    return pl.pallas_call(
        functools.partial(down_split_kernel, half),
        out_shape=jax.ShapeDtypeStruct((block_size, count, width // block_size), rows.dtype),
        in_specs=[in_vmem],
        out_specs=in_vmem,
        compiler_params=pltpu.CompilerParams(vmem_limit_bytes=12 << 20),
        name="down_split",
    )(rows)


def down_join_kernel(half, parts_ref, out_ref):
    members, _, own = parts_ref.shape
    unit = own // half
    for k in range(half):
        for member in range(members):
            at = (k * members + member) * unit
            part = parts_ref[member, :, k * unit : (k + 1) * unit]
            out_ref[:, at : at + unit] = part.astype(wide)


def down_join_units(parts, half):
    members, count, own = parts.shape
    return pl.pallas_call(
        functools.partial(down_join_kernel, half),
        out_shape=jax.ShapeDtypeStruct((count, members * own), wide),
        in_specs=[in_vmem],
        out_specs=in_vmem,
        compiler_params=pltpu.CompilerParams(vmem_limit_bytes=12 << 20),
        name="down_join",
    )(parts)


def split_kernel(half, turned_ref, grads_ref, out_ref):
    members, _, both = out_ref.shape
    unit = both // (2 * half)
    for k in range(half):
        for member in range(members):
            at = (k * members + member) * unit
            parts = [grads_ref[j, :, at : at + unit] for j in range(2)]
            for j in range(2):
                value = jnp.where(turned_ref[0] == 1, parts[1 - j], parts[j])
                out_ref[member, :, (j * half + k) * unit : (j * half + k + 1) * unit] = value


def split_columns(grads, turned, half):
    _, rows, width = grads.shape
    return pl.pallas_call(
        functools.partial(split_kernel, half),
        out_shape=jax.ShapeDtypeStruct((block_size, rows, 2 * width // block_size), grads.dtype),
        in_specs=[in_smem, in_vmem],
        out_specs=in_vmem,
        compiler_params=pltpu.CompilerParams(vmem_limit_bytes=16 << 20),
        name="split_columns",
    )(jnp.asarray(turned, jnp.int32).reshape(1), grads)


def normed(values, scales):
    return values * lax.rsqrt(jnp.mean(values * values, -1, keepdims=True) + epsilon) * scales


def gated_unit(gate, up):
    return jax.nn.gelu(gate, approximate=True) * up


def times_rows(operand, weight):
    return lax.dot_general(
        operand, weight, (((1,), (1,)), ((), ())), preferred_element_type=wide
    )


def times(operand, weight):
    return jnp.dot(operand, weight, preferred_element_type=wide)


def row_sums(gradient, operand):
    return lax.dot_general(
        gradient, operand, (((0,), (0,)), ((), ())), preferred_element_type=wide
    )


def gain_sums(gradient, weight):
    return jnp.sum(gradient * weight.astype(wide), 0)


def member_columns(values):
    rows, width = values.shape
    count = lax.axis_size("g")
    split = values.reshape(rows, count, block_size, width // (count * block_size))
    return split.transpose(2, 0, 1, 3).reshape(block_size, rows, width // block_size)


def after(values, earlier):
    return lax.optimization_barrier((values, earlier))[0]


class Exchange:
    def __init__(self, values):
        self.values = values
        self.share = 0
        self.parts = []

    def next(self, share):
        tiles = self.values.shape[0] // 16
        start = tiles * self.share // 16 * 16
        self.share += share
        return self.values, start, tiles * self.share // 16 * 16 - start

    def shift(self, share, earlier):
        values, start, size = self.next(share)
        part = lax.slice_in_dim(values, start, start + size, axis=0)
        part = after(part, earlier)
        self.parts.append(group_shift(part, 1))

    def whole(self):
        return self.parts[0] if len(self.parts) == 1 else jnp.concatenate(self.parts, 0)


def sharing(paired, plan):
    if not paired:
        return ()
    return tuple(exchange.next(share) for exchange, share in plan)


def arrived(paired, plan, parts):
    if paired:
        for (exchange, _), part in zip(plan, parts):
            exchange.parts.append(part)


def body(
    inputs,
    gain_first,
    branch_weight,
    branch_bias,
    conv_weight,
    conv_bias,
    gate_weight,
    gate_bias,
    decay,
    out_weight,
    out_bias,
    gain_second,
    mlp_weight,
    down_weight,
    cotangent,
):
    source = inputs[0].astype(wide)
    rows, width = source.shape
    heads, head_width = gate_weight.shape[1:3]
    count = lax.axis_size("g")
    half = count // 2
    paired = count == 2
    turned = (lax.axis_index("g") == 1) if paired else False
    all_rows = block_size * rows
    position = (
        lax.axis_index("g") * 4 + lax.axis_index("b3") * 2 + lax.axis_index("b2")
    ).reshape(1)
    flat = (rows, width)
    small = (8, width)

    def in_turn(first, second):
        if not paired:
            return first, second
        return jnp.where(turned, second, first), jnp.where(turned, first, second)

    def turn_halves(values):
        if not paired:
            return values
        return jnp.where(turned, jnp.roll(values, width // 2, 1), values)

    def move(gathered, swapped, collective, plan):
        outs = block_move(gathered, swapped, collective, sharing(paired, plan))
        own = (gathered is not None) + len(swapped)
        arrived(paired, plan, outs[own:])
        return outs[0] if own == 1 else outs[:own]

    def scatter(products, collective, plan, extra=None):
        out, *parts = block_scatter(products, collective, sharing(paired, plan), extra)
        arrived(paired, plan, parts)
        return out

    def joined(values, exchange):
        if paired:
            return jnp.concatenate([values, exchange.whole()], 0)
        return group_gather(values).reshape(-1, values.shape[1])

    def total(own, exchange, sums):
        if paired:
            return own + exchange.whole().astype(wide)
        return group_sum(sums)

    down_rows, hidden_width = down_weight.shape
    unit = hidden_width // (half * block_size)
    down_split = down_split_units(down_weight, half)
    mlp_trade = Exchange(mlp_weight)
    branch_trade = Exchange(branch_weight)
    out_rows = lax.all_gather(out_weight, places, axis=0, tiled=True)

    first_in = normed(source, gain_first).astype(low)
    first_all, down_own = move(
        first_in, (down_split,), 1, [(branch_trade, 16), (mlp_trade, 2)]
    )
    down_own = down_own.reshape(block_size * down_rows, half * unit)
    down_trade = Exchange(down_own)
    first_all = first_all.reshape(all_rows, width)
    cot_in = after(turn_halves(cotangent[0]), first_all)
    cot_all = lax.all_gather(cot_in, cube, axis=0, tiled=True)
    grad_out = cotangent[0]
    branch_rows = joined(branch_weight, branch_trade)
    pre_part = times_rows(first_all, branch_rows).astype(low)
    pre_part = pre_part.reshape(block_size, rows, 2 * width // block_size)
    pre = move(None, (pre_part,), 2, [(mlp_trade, 7)])
    if paired:
        mlp_trade.shift(4, pre)
    gate_pre, conv_in = joined_columns(pre, branch_bias.reshape(2, width), turned, half)
    conv_before = rim_rows(conv_in[rows - 8 :], 1)

    rate = (-8.0 * jax.nn.softplus(decay))[None]
    decays, local, product, ends = by_heads(
        local_states_kernel,
        heads,
        head_width,
        (
            position,
            conv_in,
            conv_before,
            conv_weight,
            conv_bias[None],
            gate_weight,
            gate_bias,
            rate,
        ),
        [(flat, wide)] * 3 + [((2, width), wide)],
    )
    all_ends = seq_spread(ends, 3)
    if paired:
        mlp_trade.shift(3, all_ends)
    states, mixed, entry = by_heads(
        full_states_kernel,
        heads,
        head_width,
        (position, local, product, all_ends, gate_pre),
        [(flat, wide), (flat, low), (small, wide)],
    )
    middle = source + times_rows(mixed, out_rows) + out_bias

    second_in = normed(middle, gain_second).astype(low)
    second_all = move(second_in, (), 4, [(down_trade, 12)])
    if paired:
        down_trade.shift(4, second_all)
    second_all = second_all.reshape(all_rows, width)
    if paired:
        rows_a, rows_b = mlp_weight, mlp_trade.whole()
    else:
        mlp_rows = group_gather(mlp_weight)
        rows_a = mlp_rows[:half].reshape(-1, width)
        rows_b = mlp_rows[half:].reshape(-1, width)
    down_columns = joined(down_own, down_trade)
    pre_a = times_rows(second_all, rows_a)
    mlp_gate, mlp_up = in_turn(pre_a, times_rows(second_all, rows_b))
    mlp_hidden, gated_back = jax.vjp(gated_unit, mlp_gate, mlp_up)
    mlp_hidden = mlp_hidden.astype(low)
    grad_hidden = times(cot_all, down_columns)
    grad_a, grad_b = in_turn(*(grad.astype(low) for grad in gated_back(grad_hidden)))
    sum_b = row_sums(grad_b, second_all)
    sum_b_low = sum_b.astype(low)
    mlp_back = Exchange(sum_b_low)
    grad_second = scatter(
        [(grad_a, rows_a, False), (grad_b, rows_b, False)], 5, [(mlp_back, 8)]
    )
    down_sum = row_sums(cot_all, mlp_hidden)
    down_sums = down_sum.astype(low).reshape(count, block_size * down_rows, half * unit)
    down_back = Exchange(down_sums[1])
    down_left = after(mlp_hidden, grad_second)
    down_full = scatter([(down_left, down_columns, True)], 6, [(mlp_back, 8)])
    output = (middle + turn_halves(down_full)).astype(low)[None]
    if paired:
        down_back.shift(2, down_full)

    _, second_back = jax.vjp(normed, middle, gain_second)
    grad_mid_norm, gain_second_term = second_back(grad_second)
    grad_middle = grad_out.astype(wide) + grad_mid_norm
    grad_branch = grad_middle.astype(low)
    out_bias_term = jnp.sum(grad_branch.astype(wide), 0)
    grad_mixed = times(grad_branch, out_rows)

    adjoint, tail, adjoint_ends = by_heads(
        local_adjoint_kernel,
        heads,
        head_width,
        (grad_mixed, gate_pre, decays),
        [(flat, wide), (flat, wide), ((2, width), wide)],
    )
    all_adjoint_ends = seq_spread(adjoint_ends, 9)
    mixed_all = lax.all_gather(after(mixed, down_full), cube, axis=0, tiled=True)
    if paired:
        down_back.shift(8, all_adjoint_ends)
    grad_conv, gate_weight_term, gate_sums = by_heads(
        gate_grads_kernel,
        heads,
        head_width,
        (
            position,
            adjoint,
            tail,
            all_adjoint_ends,
            decays,
            states,
            entry,
            conv_in,
            conv_before,
            conv_weight,
            conv_bias[None],
            gate_weight,
            gate_bias,
            rate,
        ),
        [(flat, wide), ((2, head_width, width), low), (small, wide)],
    )
    conv_after = rim_rows(grad_conv[:8], -1)
    pre_grads, pre_sums = by_heads(
        branch_grads_kernel,
        heads,
        head_width,
        (grad_conv, conv_after, conv_weight, gate_pre, grad_mixed, states),
        [((2, rows, width), low), (small, wide)],
    )

    columns = split_columns(pre_grads, turned, half)
    pre_all, branch_all = move(None, (columns, member_columns(grad_branch)), 10, [])
    branch_all = branch_all.reshape(all_rows, -1)
    out_sum = row_sums(branch_all, mixed_all).reshape(count, -1, width)
    out_sums = out_sum.astype(low)
    own_out, other_out = in_turn(out_sum[0], out_sum[1])
    out_back = Exchange(other_out.astype(low))
    if paired:
        down_back.shift(6, pre_all)
    pre_all = pre_all.reshape(all_rows, -1)
    branch_sum = row_sums(pre_all, first_all)
    branch_sums = branch_sum.astype(low).reshape(count, -1, width)
    branch_back = Exchange(branch_sums[1])
    gain_first_term = gain_sums(branch_sum, branch_rows)

    tops = jnp.stack([out_bias_term, gain_first_term, gain_second_term], 0)
    vectors = jnp.concatenate([gate_sums, pre_sums[:2], tops, jnp.zeros((3, width), wide)], 0)
    vectors = vectors.astype(low)
    gate_terms = gate_weight_term.reshape(block_size, -1, width)
    gate_unit = gate_terms.shape[1]
    shared_part = jnp.concatenate(
        [
            gate_terms,
            vectors[:, None, :],
            jnp.zeros((block_size, 15, width), low),
        ],
        1,
    )
    scattered = scatter(
        [(pre_all, branch_rows, False)], 11, [(branch_back, 8), (out_back, 16)], shared_part
    )
    grad_first = scattered[:rows]
    _, first_back = jax.vjp(lambda values: normed(values, gain_first), source)
    input_grad = (grad_middle + first_back(grad_first)[0])[None]
    shared = group_total(scattered[rows:]).astype(low)
    sum_a = row_sums(after(grad_a, scattered), second_all)
    mlp_low = jnp.concatenate([sum_a.astype(low), sum_b_low], 0).reshape(count, -1, width)
    mlp_grad = total(sum_a, mlp_back, mlp_low)

    if paired:
        down_total = down_sum[: block_size * down_rows] + down_back.whole().astype(wide)
    else:
        down_total = group_sum(down_sums)
    down_total = down_total.astype(low).reshape(block_size, down_rows, half * unit)
    shared_all, down_total = move(shared, (down_total,), 7, [(branch_back, 8)])
    down_grad = down_join_units(down_total, half)
    gate_sum = shared_all[:, :gate_unit].reshape(2, head_width, width)
    gate_weight_grad = jnp.stack(
        [gate_sum[:, :, h * head_width : (h + 1) * head_width] for h in range(heads)], 1
    ).astype(wide)
    sums = shared_all[:, gate_unit].astype(wide)
    branch_grad = total(branch_sum[: branch_weight.shape[0]], branch_back, branch_sums)
    out_grad = total(own_out, out_back, out_sums)
    return (
        output,
        input_grad,
        sums[11] / gain_first,
        branch_grad,
        sums[8:10].reshape(-1),
        sums[4:8],
        sums[3],
        gate_weight_grad,
        sums[:2],
        sums[2] * (-8.0 * jax.nn.sigmoid(decay)),
        out_grad,
        sums[10],
        sums[12],
        mlp_grad,
        down_grad,
    )


def solution(mesh):
    count = mesh.devices.size // block_size
    blocks = Mesh(mesh.devices.reshape((count,) + (2,) * len(cube)), places)
    tokens = P(fsdp_axes, seq_axes, None)
    owned = P(places, None)
    return jax.shard_map(
        body,
        mesh=blocks,
        in_specs=(
            tokens,
            P(),
            owned,
            P(),
            P(),
            P(),
            P(),
            P(),
            P(),
            owned,
            P(),
            P(),
            owned,
            owned,
            tokens,
        ),
        out_specs=(
            tokens,
            tokens,
            P(),
            owned,
            P(),
            P(),
            P(),
            P(),
            P(),
            P(),
            owned,
            P(),
            P(),
            owned,
            owned,
        ),
        check_vma=False,
    )
```
